1024 devices in a mesh: lat: 16 (over x, y), lon: 64 (over z, core).
Axes of the slice: x: 4, y: 4, z: 32, core: 2. Of those that a mesh axis runs over, the one named last changes fastest.
Arguments:
- pressure: float32 [16, 30, 40960], P('lat', None, 'lon'), may hold values from -6 to 6
- velocity: float32 [16, 30, 61440], P('lat', None, 'lon'), may hold values from -6 to 6
- edge_cells: int32 [16, 2, 61440], P('lat', None, 'lon'), may hold values from 0 to 1663
- cell_edges: int32 [16, 3, 40960], P('lat', None, 'lon'), may hold values from 0 to 1983
- send_cells: int32 [16, 8, 8192], P('lat', None, 'lon'), may hold values from 0 to 639
- send_edges: int32 [16, 8, 8192], P('lat', None, 'lon'), may hold values from 0 to 959
- inv_dual: float32 [16, 61440], P('lat', 'lon'), may hold values from 0.5 to 2
- edge_weight: float32 [16, 3, 40960], P('lat', None, 'lon'), may hold values from -3 to 3
- sound_speed: float32 [16, 40960], P('lat', 'lon'), may hold values from 0.1 to 0.6
- coupling: float32 [16, 30, 40960], P('lat', None, 'lon'), may hold values from 0.1 to 2
Outputs:
- pressure_out: float32 [16, 30, 40960], P('lat', None, 'lon')
- velocity_out: float32 [16, 30, 61440], P('lat', None, 'lon')
The draws below stay inside these ranges and needn't reach their ends.
Inputs may be any that keep to these rules, and one draw needn't show every extreme that they name: `edge_cells`: positions below 640 are own cells; position 640 + r * 128 + j is slot j of the halo piece from the neighbour at offset number r. `cell_edges`: positions below 960 are own edges; position 960 + r * 128 + j is slot j of the edge halo piece from the neighbour at offset number r. `send_cells`: indices of own cells. `send_edges`: indices of own edges.
All inputs are finite; a program needn't handle non-finite values.
Results may differ from the reference program's by a relative error of at most 0.0001.
Values sent between devices are 32-bit elements; how exact they have to be, the bound alone decides.
A program may use at most 64 MiB of HBM per device.

```python
import math
import jax
import jax.numpy as jnp
from jax import lax

C_DEV = 640
E_DEV = 960
HALO = 128
NLEV = 30
NSUB = 3
CELLS_ROW = 40960
EDGES_ROW = 61440
SLOTS_ROW = 8192
N_LAT = 16
N_LON = 64


def with_ends(values, own_key, smallest, largest):
    spot = [jax.random.randint(jax.random.fold_in(own_key, axis), (), 0, length) for axis, length in enumerate(values.shape)]
    longest = values.shape.index(max(values.shape))
    neighbour = spot[:longest] + [(spot[longest] + 1) % values.shape[longest]] + spot[longest + 1:]
    return values.at[tuple(spot)].set(smallest).at[tuple(neighbour)].set(largest)


def block_levels(own_key, dims, cuts, low, top_value):
    factor_of, own = 1.0, jax.random.fold_in(own_key, 6)
    for dim, shards_of in cuts:
        heights = jnp.exp(jax.random.uniform(jax.random.fold_in(own, dim), (shards_of,), jnp.float32, low / len(cuts), top_value / len(cuts)))
        factor_of = factor_of * jnp.repeat(heights, dims[dim] // shards_of).reshape([-1 if axis == dim else 1 for axis in range(len(dims))])
    return factor_of


def normal_values(rng, extent, scale, bound, cuts=(), kind=jnp.bfloat16):
    values = scale * jax.random.normal(rng, extent, jnp.float32)
    if cuts:
        values = values * block_levels(rng, extent, cuts, -0.22, 0.18)
    return jnp.clip(values, -bound, bound).astype(kind)


def setup_inputs(seed: int = 0) -> dict:
    streams_of = jax.random.split(jax.random.key(seed), 11)
    return {
        "pressure": normal_values(streams_of[0], (N_LAT, NLEV, CELLS_ROW), 1.0, 6.0, ((0, 16), (2, 64)), jnp.float32),
        "velocity": normal_values(streams_of[1], (N_LAT, NLEV, EDGES_ROW), 1.0, 6.0, ((0, 16), (2, 64)), jnp.float32),
        "edge_cells": with_ends(jax.random.randint(streams_of[2], (N_LAT, 2, EDGES_ROW), 0, C_DEV + 8 * HALO), jax.random.fold_in(streams_of[2], 1), 0, (C_DEV + 8 * HALO) - 1).astype(jnp.int32),
        "cell_edges": with_ends(jax.random.randint(streams_of[3], (N_LAT, 3, CELLS_ROW), 0, E_DEV + 8 * HALO), jax.random.fold_in(streams_of[3], 1), 0, (E_DEV + 8 * HALO) - 1).astype(jnp.int32),
        "send_cells": with_ends(jax.random.randint(streams_of[4], (N_LAT, 8, SLOTS_ROW), 0, C_DEV), jax.random.fold_in(streams_of[4], 1), 0, C_DEV - 1).astype(jnp.int32),
        "send_edges": with_ends(jax.random.randint(streams_of[5], (N_LAT, 8, SLOTS_ROW), 0, E_DEV), jax.random.fold_in(streams_of[5], 1), 0, E_DEV - 1).astype(jnp.int32),
        "inv_dual": jnp.clip(jnp.exp(math.log(2.0) - 1.3862944 * jax.random.uniform(streams_of[6], (N_LAT, EDGES_ROW), jnp.float32) ** block_levels(streams_of[6], (N_LAT, EDGES_ROW), ((0, 16), (1, 64)), -0.2, 0.2)), 0.5, 2.0),
        "edge_weight": normal_values(streams_of[7], (N_LAT, 3, CELLS_ROW), 0.5, 3.0, ((0, 16), (2, 64)), jnp.float32),
        "sound_speed": jnp.clip(jnp.exp(math.log(0.6) - 1.7917595 * jax.random.uniform(streams_of[8], (N_LAT, CELLS_ROW), jnp.float32) ** block_levels(streams_of[8], (N_LAT, CELLS_ROW), ((0, 16), (1, 64)), -0.2, 0.2)), 0.1, 0.6),
        "coupling": jnp.clip(jnp.exp(math.log(2.0) - 2.9957323 * jax.random.uniform(streams_of[9], (N_LAT, NLEV, CELLS_ROW), jnp.float32) ** block_levels(streams_of[9], (N_LAT, NLEV, CELLS_ROW), ((0, 16), (2, 64)), -0.2, 0.2)), 0.1, 2.0),
    }


DIRECTIONS = ((-1, -1), (-1, 0), (-1, 1), (0, -1), (0, 1), (1, -1), (1, 0), (1, 1))
step_scale = 0.5


def position(offset):
    return DIRECTIONS.index(offset)


def edge_update(normal, extended, edge_cells, inv_dual):
    gradient = (jnp.take(extended, edge_cells[1], axis=1) - jnp.take(extended, edge_cells[0], axis=1)) * inv_dual[None, :]
    return normal - step_scale * gradient


def column_solve(right_side, coupling):
    levels = right_side.shape[0]
    ratios = []
    scaled = []
    for level_index in range(levels):
        if level_index < levels - 1:
            upper_term = -coupling[level_index]
        else:
            upper_term = 0.0 * coupling[0]
        if level_index == 0:
            divisor = 1.0 + coupling[0]
            current = right_side[0] / divisor
        else:
            lower_term = -coupling[level_index - 1]
            diagonal = 1.0 + coupling[level_index - 1] + coupling[level_index]
            divisor = diagonal - lower_term * ratios[-1]
            current = (right_side[level_index] - lower_term * scaled[-1]) / divisor
        ratios.append(upper_term / divisor)
        scaled.append(current)
    result = [scaled[-1]]
    for level_index in range(levels - 2, -1, -1):
        result.insert(0, scaled[level_index] - ratios[level_index] * result[0])
    return jnp.stack(result)


def cell_update(values, edges_ext, cell_edges, edge_weight, sound_speed, coupling):
    divergence = jnp.take(edges_ext, cell_edges[0], axis=1) * edge_weight[0][None, :]
    divergence = divergence + jnp.take(edges_ext, cell_edges[1], axis=1) * edge_weight[1][None, :]
    divergence = divergence + jnp.take(edges_ext, cell_edges[2], axis=1) * edge_weight[2][None, :]
    right_side = values - sound_speed[None, :] * divergence
    return column_solve(right_side, coupling)


def device_layout(array, width):
    if array.ndim == 2:
        return array.reshape(N_LAT, N_LON, width)
    return array.reshape(N_LAT, array.shape[1], N_LON, width).transpose(0, 2, 1, 3)


def global_layout(array):
    return array.transpose(0, 2, 1, 3).reshape(N_LAT, array.shape[2], N_LON * array.shape[3])


def take_pieces(source, indices):
    return jnp.take(source, indices, axis=1)


def reference_extend(source, send_list):
    taker = jax.vmap(jax.vmap(take_pieces))
    pieces = []
    for offset in DIRECTIONS:
        piece = taker(source, send_list[:, :, position((-offset[0], -offset[1]))])
        piece = jnp.roll(piece, -offset[1], axis=1)
        if offset[0] == 1:
            piece = jnp.concatenate([piece[1:], jnp.zeros_like(piece[:1])], axis=0)
        elif offset[0] == -1:
            piece = jnp.concatenate([jnp.zeros_like(piece[:1]), piece[:-1]], axis=0)
        pieces.append(piece)
    return jnp.concatenate([source] + pieces, axis=3)


def band_edges(operands):
    return jax.vmap(edge_update)(*operands)


def band_cells(operands):
    return jax.vmap(cell_update)(*operands)


def reference(pressure, velocity, edge_cells, cell_edges, send_cells, send_edges, inv_dual, edge_weight, sound_speed, coupling):
    values = device_layout(pressure, C_DEV)
    normal = device_layout(velocity, E_DEV)
    edge_pairs = device_layout(edge_cells, E_DEV)
    cell_sides = device_layout(cell_edges, C_DEV)
    cell_lists = device_layout(send_cells, HALO)
    edge_lists = device_layout(send_edges, HALO)
    inverse = device_layout(inv_dual, E_DEV)
    weights = device_layout(edge_weight, C_DEV)
    speeds = device_layout(sound_speed, C_DEV)
    couples = device_layout(coupling, C_DEV)
    for substep in range(NSUB):
        extended = reference_extend(values, cell_lists)
        normal = lax.map(band_edges, (normal, extended, edge_pairs, inverse))
        edges_ext = reference_extend(normal, edge_lists)
        values = lax.map(band_cells, (values, edges_ext, cell_sides, weights, speeds, couples))
    return global_layout(values), global_layout(normal)
```

```python
import functools

import jax
import jax.numpy as jnp
from jax import lax
from jax.experimental import pallas as pl
from jax.experimental.pallas import tpu as pltpu
from jax.sharding import PartitionSpec as P

NSUB = 3
C = 640
E = 960
EP = 1024
H = 128
L = 30
LP = 32
N = 8 * H
DIRECTIONS = ((-1, -1), (-1, 0), (-1, 1), (0, -1), (0, 1), (1, -1), (1, 0), (1, 1))
ORDER = (0, 2, 5, 7, 1, 6, 3, 4)
F32, BF16 = jnp.float32, jnp.bfloat16
MESH = pl.DeviceIdType.MESH


def split(x):
    high = x.astype(BF16)
    return high, (x - high.astype(F32)).astype(BF16)


def dot(a, b):
    return jnp.dot(a, b, preferred_element_type=F32)


def halves(x):
    return x[:LP] + x[LP:]


def kernel(
    n_lat, n_lon,
    p_hbm, v_hbm, ec_hbm, ce_hbm, sc_hbm, se_hbm, inv_hbm, w_hbm, ss_hbm, cp_hbm,
    p_out, v_out,
    p_in, v_in, ec_in, ce_in, sc_in, se_in, inv_in, w_in, ss_in, cp_in,
    pres, vel, pieces_out, pieces_in,
    pres_hl, vel_hl, pick_c, pick_e, diff, diff_l, weight,
    rows_l, grad_l, vel_l, right, solve_in, solve_mid, coef_a, coef_b, coef_r,
    in_sem, out_sem, send_sem, recv_sem,
):
    a, b = lax.axis_index("lat"), lax.axis_index("lon")
    not_first, not_last = a > 0, a < n_lat - 1

    def neighbour(member):
        p, q = DIRECTIONS[member]
        return (a + p, lax.rem(b + q + n_lon, n_lon))

    barrier = pltpu.get_barrier_semaphore()

    def greet(members):
        for member in members:
            pl.semaphore_signal(barrier, inc=1, device_id=neighbour(member), device_id_type=MESH)

    greet((3, 4))
    pl.when(not_first)(lambda: greet((0, 1, 2)))
    pl.when(not_last)(lambda: greet((5, 6, 7)))

    sources = (sc_hbm, p_hbm, se_hbm, v_hbm, ec_hbm, inv_hbm, ce_hbm, w_hbm, ss_hbm, cp_hbm)
    targets = (sc_in, p_in, se_in, v_in, ec_in, inv_in, ce_in, w_in, ss_in, cp_in)
    loads = []
    for i, (source, target) in enumerate(zip(sources, targets)):
        view = source if source.ndim == 2 else source.at[0]
        loads.append(pltpu.make_async_copy(view, target, in_sem.at[i]))
        loads[-1].start()

    def copy(exchange, member):
        return pltpu.make_async_remote_copy(
            src_ref=pieces_out.at[exchange, member],
            dst_ref=pieces_in.at[exchange, 7 - member],
            send_sem=send_sem.at[exchange, member],
            recv_sem=recv_sem.at[exchange, 7 - member],
            device_id=neighbour(member),
            device_id_type=MESH,
        )

    def by_row(members, action):
        for member in members:
            row = DIRECTIONS[member][0]
            if row == 0:
                action(member)
            else:
                pl.when(not_first if row < 0 else not_last)(functools.partial(action, member))

    def receive(exchange, members, target, base):
        for member in members:
            pltpu.make_async_remote_copy(
                src_ref=pieces_out.at[exchange, member],
                dst_ref=pieces_in.at[exchange, member],
                send_sem=send_sem.at[exchange, member],
                recv_sem=recv_sem.at[exchange, member],
                device_id=neighbour(member),
                device_id_type=MESH,
            ).wait_recv()
        for member in members:
            high, low = split(pieces_in[exchange, member])
            target[:LP, base + member * H:base + (member + 1) * H] = high
            target[LP:, base + member * H:base + (member + 1) * H] = low

    def receive_rest(exchange, target, base):
        pl.when(not_first)(lambda: receive(exchange, (0, 1, 2), target, base))
        pl.when(not_last)(lambda: receive(exchange, (5, 6, 7), target, base))

    def one_hot_rows(start, count, width):
        return (lax.broadcasted_iota(jnp.int32, (count, width), 0) + start).astype(F32)

    def build_pick(lists_ref, target, own):
        lists = lists_ref[...].astype(F32)
        picks = jnp.concatenate([lists[member:member + 1] for member in ORDER], axis=1)

        def step(i, carry):
            start = pl.multiple_of(i * 32, 32)
            hit = one_hot_rows(start, 32, N) == picks
            target[pl.ds(start, 32), :] = jnp.where(hit, 1.0, 0.0).astype(BF16)
            return carry

        lax.fori_loop(0, own // 32, step, 0)

    def build_diff(first, second, target):
        def step(i, carry):
            start = pl.multiple_of(i * 32, 32)
            rows = one_hot_rows(start, 32, N)
            hit = jnp.where(rows == second, 1.0, 0.0) - jnp.where(rows == first, 1.0, 0.0)
            target[pl.ds(start, 32), :] = hit.astype(BF16)
            return carry

        lax.fori_loop(0, (C + N) // 32, step, 0)

    def build_weight():
        places = ce_in[...].astype(F32)
        places = jnp.where(places >= E, places + (EP - E), places)
        weights = w_in[...] * ss_in[...]

        def step(i, carry):
            start = pl.multiple_of(i * 32, 32)
            rows = one_hot_rows(start, 32, C)
            total = jnp.where(rows == places[0:1], weights[0:1], 0.0)
            total = total + jnp.where(rows == places[1:2], weights[1:2], 0.0)
            total = total + jnp.where(rows == places[2:3], weights[2:3], 0.0)
            high, low = split(total)
            weight[pl.ds(start, 32), :C] = high
            weight[pl.ds(start, 32), C:] = low
            return carry

        lax.fori_loop(0, (EP + N) // 32, step, 0)

    def to_columns(x, target):
        for block in range(C // H):
            target[pl.ds(block, LP, stride=8), :] = x[:, block * H:(block + 1) * H]

    def build_solver():
        coupling = jnp.concatenate([cp_in[...], jnp.zeros((LP - L, C), F32)], axis=0)
        to_columns(coupling, solve_in)
        below, inverse = None, None
        for k in range(L):
            here = solve_in[8 * k:8 * k + 8, :]
            divisor = 1.0 + here
            if k > 0:
                divisor = divisor + below - below * (below * inverse)
            inverse = 1.0 / divisor
            coef_a[8 * k:8 * k + 8, :] = inverse
            if k > 0:
                coef_b[8 * k:8 * k + 8, :] = below * inverse
            coef_r[8 * k:8 * k + 8, :] = here * inverse
            below = here

    def solve():
        current = solve_in[0:8, :] * coef_a[0:8, :]
        solve_mid[0:8, :] = current
        for k in range(1, L):
            rows = slice(8 * k, 8 * k + 8)
            current = solve_in[rows, :] * coef_a[rows, :] + coef_b[rows, :] * current
            solve_mid[rows, :] = current
        for k in range(L - 2, -1, -1):
            rows = slice(8 * k, 8 * k + 8)
            current = solve_mid[rows, :] + coef_r[rows, :] * current
            solve_mid[rows, :] = current
        for block in range(C // H):
            x = solve_mid[pl.ds(block, LP, stride=8), :]
            pres[:, block * H:(block + 1) * H] = x
            high, low = split(x)
            pres_hl[:LP, block * H:(block + 1) * H] = high
            pres_hl[LP:, block * H:(block + 1) * H] = low

    def pressure_pieces(exchange):
        for chunk in range(4):
            cols = slice(chunk * 256, chunk * 256 + 256)
            picked = halves(dot(pres_hl[:, :C], pick_c[:, cols]))
            for half in range(2):
                pieces_out[exchange, ORDER[2 * chunk + half]] = picked[:, half * H:(half + 1) * H]

    def own_gradient():
        for chunk in range(4):
            cols = slice(chunk * 256, chunk * 256 + 256)
            grad_l[:, cols] = halves(dot(pres_hl[:, :C], diff_l[:C, cols]))

    loads[0].wait()
    build_pick(sc_in, pick_c, C)
    loads[1].wait()
    start = jnp.concatenate([p_in[...], jnp.zeros((LP - L, C), F32)], axis=0)
    pres[...] = start
    high, low = split(start)
    pres_hl[:LP, :C] = high
    pres_hl[LP:, :C] = low
    pres_hl[:, C:] = jnp.zeros((2 * LP, N), BF16)
    pressure_pieces(0)
    pl.semaphore_wait(barrier, 2 + 3 * lax.min(a, 1) + 3 * lax.min(n_lat - 1 - a, 1))
    by_row(ORDER, lambda member: copy(0, member).start())

    loads[2].wait()
    build_pick(se_in, pick_e, EP)
    for i in range(3, 10):
        loads[i].wait()
    vel[...] = jnp.zeros_like(vel)
    vel[:L, :E] = v_in[...]
    high, low = split(vel[...])
    vel_hl[:LP, :EP] = high
    vel_hl[LP:, :EP] = low
    vel_hl[:, EP:] = jnp.zeros((2 * LP, N), BF16)
    rows_l[...] = jnp.full(rows_l.shape, -1.0, F32)
    rows_l[0:2, :E] = ec_in[...].astype(F32)
    rows_l[2:3, :] = jnp.zeros((1, EP), F32)
    rows_l[2:3, :E] = 0.5 * inv_in[...]
    own_rows = rows_l[...]
    cells_first, cells_second, factor = own_rows[0:1], own_rows[1:2], own_rows[2:3]
    coarse = jnp.floor(own_rows[0:2] * (1.0 / H))
    fine = own_rows[0:2] - H * coarse
    factor_high = factor.astype(BF16).astype(F32)
    factor_mid = (factor - factor_high).astype(BF16).astype(F32)
    factor_low = factor - factor_high - factor_mid
    parts = jnp.concatenate(
        [coarse, fine, factor_high, factor_mid, factor_low, jnp.zeros((9, EP), F32)], axis=0
    ).astype(BF16)
    for chunk in range(4):
        cols = slice(chunk * 256, chunk * 256 + 256)
        vel_l[:, cols] = halves(dot(vel_hl[:, :EP], pick_e[:, cols]))
        found = dot(parts, pick_e[:, cols])
        rows_l[4:6, cols] = found[0:2] * H + found[2:4]
        rows_l[6:7, cols] = found[4:5] + found[5:6] + found[6:7]
    sent_rows = rows_l[...]
    build_diff(sent_rows[4:5], sent_rows[5:6], diff_l)
    own_gradient()
    build_diff(cells_first, cells_second, diff)

    def substep(s, carry):
        first, second = 2 * s, 2 * s + 1
        receive(first, (3, 4), pres_hl, C)
        near = slice(C + 3 * H, C + 5 * H)
        for chunk in range(4):
            cols = slice(chunk * 256, chunk * 256 + 256)
            grad_l[:, cols] = grad_l[:, cols] + halves(dot(pres_hl[:, near], diff_l[near, cols]))
        receive_rest(first, pres_hl, C)
        behind, ahead = slice(C, C + 3 * H), slice(C + 5 * H, C + 8 * H)
        for chunk in range(4):
            cols = slice(chunk * 256, chunk * 256 + 256)
            far = dot(pres_hl[:, behind], diff_l[behind, cols])
            far = far + dot(pres_hl[:, ahead], diff_l[ahead, cols])
            moved = vel_l[:, cols] - rows_l[6:7, cols] * (grad_l[:, cols] + halves(far))
            vel_l[:, cols] = moved
            for half in range(2):
                pieces_out[second, ORDER[2 * chunk + half]] = moved[:, half * H:(half + 1) * H]
            by_row(ORDER[2 * chunk:2 * chunk + 2], lambda member: copy(second, member).start())

        for chunk in range(4):
            cols = slice(chunk * 256, chunk * 256 + 256)
            gradient = halves(dot(pres_hl[...], diff[:, cols]))
            moved = vel[:, cols] - rows_l[2:3, cols] * gradient
            vel[:, cols] = moved
            high, low = split(moved)
            vel_hl[:LP, cols] = high
            vel_hl[LP:, cols] = low

        @pl.when(s == 0)
        def _():
            build_weight()
            build_solver()

        @pl.when(s == NSUB - 1)
        def _():
            v_in[...] = vel[:L, :E]
            pltpu.make_async_copy(v_in, v_out.at[0], out_sem.at[0]).start()

        def divergence(places):
            wide = dot(vel_hl[:, places], weight[places, :])
            return halves(wide[:, :C] + wide[:, C:])

        right[...] = pres[...] - divergence(slice(0, EP))
        receive(second, (3, 4), vel_hl, EP)
        right[...] = right[...] - divergence(slice(EP + 3 * H, EP + 5 * H))
        receive_rest(second, vel_hl, EP)
        total = divergence(slice(EP, EP + 3 * H)) + divergence(slice(EP + 5 * H, EP + 8 * H))
        to_columns(right[...] - total, solve_in)
        solve()

        @pl.when(s < NSUB - 1)
        def _():
            pressure_pieces(second + 1)
            by_row(ORDER, lambda member: copy(second + 1, member).start())
            own_gradient()

        return carry

    lax.fori_loop(0, NSUB, substep, 0)
    p_in[...] = pres[:L, :]
    pressure_store = pltpu.make_async_copy(p_in, p_out.at[0], out_sem.at[1])
    pressure_store.start()
    for exchange in range(2 * NSUB):
        by_row(ORDER, lambda member: copy(exchange, member).wait_send())
    pltpu.make_async_copy(v_in, v_out.at[0], out_sem.at[0]).wait()
    pressure_store.wait()


def solution(mesh):
    n_lat, n_lon = mesh.shape["lat"], mesh.shape["lon"]
    any_space = pl.BlockSpec(memory_space=pl.ANY)
    vmem = pltpu.VMEM
    i32 = jnp.int32

    def on_device(*operands):
        return pl.pallas_call(
            functools.partial(kernel, n_lat, n_lon),
            out_shape=(
                jax.ShapeDtypeStruct((1, L, C), F32),
                jax.ShapeDtypeStruct((1, L, E), F32),
            ),
            in_specs=[any_space] * 10,
            out_specs=(any_space, any_space),
            scratch_shapes=[
                vmem((L, C), F32), vmem((L, E), F32),
                vmem((2, E), i32), vmem((3, C), i32), vmem((8, H), i32), vmem((8, H), i32),
                vmem((1, E), F32), vmem((3, C), F32), vmem((1, C), F32), vmem((L, C), F32),
                vmem((LP, C), F32), vmem((LP, EP), F32),
                vmem((2 * NSUB, 8, LP, H), F32), vmem((2 * NSUB, 8, LP, H), F32),
                vmem((2 * LP, C + N), BF16), vmem((2 * LP, EP + N), BF16),
                vmem((C, N), BF16), vmem((EP, N), BF16),
                vmem((C + N, N), BF16), vmem((C + N, N), BF16), vmem((EP + N, 2 * C), BF16),
                vmem((8, N), F32), vmem((LP, N), F32), vmem((LP, N), F32), vmem((LP, C), F32),
                vmem((8 * LP, H), F32), vmem((8 * LP, H), F32),
                vmem((8 * LP, H), F32), vmem((8 * LP, H), F32), vmem((8 * LP, H), F32),
                pltpu.SemaphoreType.DMA((10,)), pltpu.SemaphoreType.DMA((2,)),
                pltpu.SemaphoreType.DMA((2 * NSUB, 8)), pltpu.SemaphoreType.DMA((2 * NSUB, 8)),
            ],
            compiler_params=pltpu.CompilerParams(
                collective_id=0, has_side_effects=True, vmem_limit_bytes=60 * 1024 * 1024
            ),
        )(*operands)

    spec3, spec2 = P("lat", None, "lon"), P("lat", "lon")
    return jax.shard_map(
        on_device,
        mesh=mesh,
        in_specs=(spec3, spec3, spec3, spec3, spec3, spec3, spec2, spec3, spec2, spec3),
        out_specs=(spec3, spec3),
        check_vma=False,
    )
```

```python
import functools

import jax
import jax.numpy as jnp
from jax import lax
from jax.experimental import pallas as pl
from jax.experimental.pallas import tpu as pltpu
from jax.sharding import PartitionSpec as P

NSUB = 3
C = 640
E = 960
EP = 1024
H = 128
L = 30
LP = 32
N = 8 * H
DIRECTIONS = ((-1, -1), (-1, 0), (-1, 1), (0, -1), (0, 1), (1, -1), (1, 0), (1, 1))
F32, BF16 = jnp.float32, jnp.bfloat16
MESH = pl.DeviceIdType.MESH


def split(x):
    high = x.astype(BF16)
    return high, (x - high.astype(F32)).astype(BF16)


def dot(a, b):
    return jnp.dot(a, b, preferred_element_type=F32)


def halves(x):
    return x[:LP] + x[LP:]


def kernel(
    n_lat, n_lon,
    p_hbm, v_hbm, ec_hbm, ce_hbm, sc_hbm, se_hbm, inv_hbm, w_hbm, ss_hbm, cp_hbm,
    p_out, v_out,
    p_in, v_in, ec_in, ce_in, sc_in, se_in, inv_in, w_in, ss_in, cp_in,
    pres, vel, pieces_out, pieces_in,
    pres_hl, vel_hl, pick_c, pick_e, diff, diff_l, weight,
    rows_l, grad_l, vel_l, right, solve_in, solve_mid, coef_a, coef_b, coef_r,
    in_sem, send_sem, recv_sem,
):
    a, b = lax.axis_index("lat"), lax.axis_index("lon")
    not_first, not_last = a > 0, a < n_lat - 1

    def device_at(p, q):
        return (a + p, lax.rem(b + q + n_lon, n_lon))

    def neighbour(member):
        return device_at(*DIRECTIONS[member])

    core = lax.rem(b, 2)
    cross = 2 * core - 1
    order = (
        (-1, cross, 2 * core), (1, cross, 5 + 2 * core),
        (-1, -cross, 2 - 2 * core), (1, -cross, 7 - 2 * core),
        (-1, 0, 1), (1, 0, 6), (0, cross, 3 + core), (0, -cross, 4 - core),
    )

    barrier = pltpu.get_barrier_semaphore()

    def greet(members):
        for member in members:
            pl.semaphore_signal(barrier, inc=1, device_id=neighbour(member), device_id_type=MESH)

    greet((3, 4))
    pl.when(not_first)(lambda: greet((0, 1, 2)))
    pl.when(not_last)(lambda: greet((5, 6, 7)))

    sources = (sc_hbm, p_hbm, se_hbm, v_hbm, ec_hbm, inv_hbm, ce_hbm, w_hbm, ss_hbm, cp_hbm)
    targets = (sc_in, p_in, se_in, v_in, ec_in, inv_in, ce_in, w_in, ss_in, cp_in)
    loads = []
    for i, (source, target) in enumerate(zip(sources, targets)):
        if source.ndim == 2:
            view = source
        else:
            view = source.at[0] if source.shape[0] == 1 else source.at[:, 0, :]
        loads.append(pltpu.make_async_copy(view, target, in_sem.at[i]))
        loads[-1].start()

    def copy(exchange, turn):
        p, q, member = order[turn]
        return pltpu.make_async_remote_copy(
            src_ref=pieces_out.at[exchange, turn],
            dst_ref=pieces_in.at[exchange, 7 - member],
            send_sem=send_sem.at[exchange, turn],
            recv_sem=recv_sem.at[exchange, 7 - member],
            device_id=device_at(p, q),
            device_id_type=MESH,
        )

    def each(turns, action):
        for turn in turns:
            row = order[turn][0]
            if row == 0:
                action(turn)
            else:
                pl.when(not_first if row < 0 else not_last)(functools.partial(action, turn))

    def send(exchange, turns):
        each(turns, lambda turn: copy(exchange, turn).start())

    def receive(exchange, members, target, base):
        for member in members:
            pltpu.make_async_remote_copy(
                src_ref=pieces_out.at[exchange, member],
                dst_ref=pieces_in.at[exchange, member],
                send_sem=send_sem.at[exchange, member],
                recv_sem=recv_sem.at[exchange, member],
                device_id=neighbour(member),
                device_id_type=MESH,
            ).wait_recv()
        for member in members:
            high, low = split(pieces_in[exchange, member])
            target[:L, base + member * H:base + (member + 1) * H] = high
            target[LP:LP + L, base + member * H:base + (member + 1) * H] = low

    def receive_rest(exchange, target, base):
        pl.when(not_first)(lambda: receive(exchange, (0, 1, 2), target, base))
        pl.when(not_last)(lambda: receive(exchange, (5, 6, 7), target, base))

    def in_blocks(count, build):
        def step(block, carry):
            start = pl.multiple_of(block * H, H)
            base = start.astype(F32)

            def local(places):
                within = places - base
                within = jnp.where((within >= 0.0) & (within < float(H)), within, -1.0)
                return jnp.broadcast_to(within, (16, places.shape[1])).astype(BF16)

            build(start, local)
            return carry

        lax.fori_loop(0, count // H, step, 0)

    def row_numbers(j, width):
        return (lax.broadcasted_iota(jnp.int32, (16, width), 0) + 16 * j).astype(F32).astype(BF16)

    def build_pick(lists_ref, target, own):
        lists = lists_ref[...].astype(F32)

        def either(first, second):
            return jnp.where(core == 0, lists[first:first + 1], lists[second:second + 1])

        picks = jnp.concatenate(
            [either(0, 2), either(5, 7), either(2, 0), either(7, 5),
             lists[1:2], lists[6:7], either(3, 4), either(4, 3)], axis=1)

        def build(start, local):
            here = local(picks)
            one, zero = jnp.ones((16, N), BF16), jnp.zeros((16, N), BF16)
            for j in range(H // 16):
                target[pl.ds(start + 16 * j, 16), :] = jnp.where(row_numbers(j, N) == here, one, zero)

        in_blocks(own, build)

    def build_diff(first, second, target):
        def build(start, local):
            minus, plus = local(first), local(second)
            one, zero = jnp.ones((16, N), BF16), jnp.zeros((16, N), BF16)
            for j in range(H // 16):
                rows = row_numbers(j, N)
                hit = jnp.where(rows == plus, one, zero) - jnp.where(rows == minus, one, zero)
                target[pl.ds(start + 16 * j, 16), :] = hit

        in_blocks(C + N, build)

    def build_weight():
        places = ce_in[...].astype(F32)
        places = jnp.where(places >= E, places + (EP - E), places)
        weights = w_in[...] * ss_in[...]
        place = [places[j:j + 1] for j in range(3)]
        factor = [weights[j:j + 1] for j in range(3)]
        for i, j in ((0, 1), (0, 2), (1, 2)):
            same = place[i] == place[j]
            factor[i] = factor[i] + jnp.where(same, factor[j], 0.0)
            place[j] = jnp.where(same, -1.0, place[j])
        parts = [split(jnp.broadcast_to(x, (16, C))) for x in factor]

        def build(start, local):
            here = [local(x) for x in place]
            zero = jnp.zeros((16, C), BF16)
            for j in range(H // 16):
                rows = row_numbers(j, C)
                high, low = zero, zero
                for where, (part_high, part_low) in zip(here, parts):
                    hit = rows == where
                    high, low = jnp.where(hit, part_high, high), jnp.where(hit, part_low, low)
                weight[pl.ds(start + 16 * j, 16), :C] = high
                weight[pl.ds(start + 16 * j, 16), C:] = low

        in_blocks(EP + N, build)

    def to_columns(x, target):
        for block in range(C // H):
            target[pl.ds(block, LP, stride=8), :] = x[:, block * H:(block + 1) * H]

    def build_solver():
        coupling = jnp.concatenate([cp_in[...], jnp.zeros((LP - L, C), F32)], axis=0)
        to_columns(coupling, solve_in)
        below, inverse = None, None
        for k in range(L):
            here = solve_in[8 * k:8 * k + 8, :]
            divisor = 1.0 + here
            if k > 0:
                divisor = divisor + below - below * (below * inverse)
            inverse = 1.0 / divisor
            coef_a[8 * k:8 * k + 8, :] = inverse
            if k > 0:
                coef_b[8 * k:8 * k + 8, :] = below * inverse
            coef_r[8 * k:8 * k + 8, :] = here * inverse
            below = here

    def solve():
        current = solve_in[0:8, :] * coef_a[0:8, :]
        solve_mid[0:8, :] = current
        for k in range(1, L):
            rows = slice(8 * k, 8 * k + 8)
            current = solve_in[rows, :] * coef_a[rows, :] + coef_b[rows, :] * current
            solve_mid[rows, :] = current
        for k in range(L - 2, -1, -1):
            rows = slice(8 * k, 8 * k + 8)
            current = solve_mid[rows, :] + coef_r[rows, :] * current
            solve_mid[rows, :] = current
        for block in range(C // H):
            x = solve_mid[pl.ds(block, LP, stride=8), :]
            pres[:, block * H:(block + 1) * H] = x
            high, low = split(x)
            pres_hl[:LP, block * H:(block + 1) * H] = high
            pres_hl[LP:, block * H:(block + 1) * H] = low

    def put_pieces(exchange, chunk, x):
        for half in range(2):
            pieces_out[exchange, 2 * chunk + half] = x[:L, half * H:(half + 1) * H]

    def pressure_pieces(exchange, at_once):
        for chunk in range(4):
            cols = slice(chunk * 256, chunk * 256 + 256)
            put_pieces(exchange, chunk, halves(dot(pres_hl[:, :C], pick_c[:, cols])))
            if at_once:
                send(exchange, (2 * chunk, 2 * chunk + 1))

    def own_gradient():
        for chunk in range(4):
            cols = slice(chunk * 256, chunk * 256 + 256)
            grad_l[:, cols] = halves(dot(pres_hl[:, :C], diff_l[:C, cols]))

    loads[0].wait()
    build_pick(sc_in, pick_c, C)
    loads[1].wait()
    start = jnp.concatenate([p_in[...], jnp.zeros((LP - L, C), F32)], axis=0)
    pres[...] = start
    high, low = split(start)
    pres_hl[:LP, :C] = high
    pres_hl[LP:, :C] = low
    pres_hl[:, C:] = jnp.zeros((2 * LP, N), BF16)
    pressure_pieces(0, False)
    pl.semaphore_wait(barrier, 2 + 3 * lax.min(a, 1) + 3 * lax.min(n_lat - 1 - a, 1))
    send(0, range(8))

    loads[2].wait()
    build_pick(se_in, pick_e, EP)
    for i in range(3, 10):
        loads[i].wait()
    vel[...] = jnp.zeros_like(vel)
    vel[:L, :E] = v_in[...]
    high, low = split(vel[...])
    vel_hl[:LP, :EP] = high
    vel_hl[LP:, :EP] = low
    vel_hl[:, EP:] = jnp.zeros((2 * LP, N), BF16)
    rows_l[...] = jnp.full(rows_l.shape, -1.0, F32)
    rows_l[0:2, :E] = ec_in[...].astype(F32)
    rows_l[2:3, :] = jnp.zeros((1, EP), F32)
    rows_l[2:3, :E] = 0.5 * inv_in[...]
    own_rows = rows_l[...]
    cells_first, cells_second, factor = own_rows[0:1], own_rows[1:2], own_rows[2:3]
    coarse = jnp.floor(own_rows[0:2] * (1.0 / H))
    fine = own_rows[0:2] - H * coarse
    factor_high = factor.astype(BF16).astype(F32)
    factor_mid = (factor - factor_high).astype(BF16).astype(F32)
    factor_low = factor - factor_high - factor_mid
    parts = jnp.concatenate(
        [coarse, fine, factor_high, factor_mid, factor_low, jnp.zeros((9, EP), F32)], axis=0
    ).astype(BF16)
    for chunk in range(4):
        cols = slice(chunk * 256, chunk * 256 + 256)
        vel_l[:, cols] = halves(dot(vel_hl[:, :EP], pick_e[:, cols]))
        found = dot(parts, pick_e[:, cols])
        rows_l[4:6, cols] = found[0:2] * H + found[2:4]
        rows_l[6:7, cols] = found[4:5] + found[5:6] + found[6:7]
    sent_rows = rows_l[...]
    build_diff(sent_rows[4:5], sent_rows[5:6], diff_l)
    own_gradient()
    build_diff(cells_first, cells_second, diff)

    def substep(s, carry):
        first, second = 2 * s, 2 * s + 1
        receive(first, (3, 4), pres_hl, C)
        near = slice(C + 3 * H, C + 5 * H)
        for chunk in range(4):
            cols = slice(chunk * 256, chunk * 256 + 256)
            grad_l[:, cols] = grad_l[:, cols] + halves(dot(pres_hl[:, near], diff_l[near, cols]))
        receive_rest(first, pres_hl, C)
        behind, ahead = slice(C, C + 3 * H), slice(C + 5 * H, C + 8 * H)
        for chunk in range(4):
            cols = slice(chunk * 256, chunk * 256 + 256)
            far = dot(pres_hl[:, behind], diff_l[behind, cols])
            far = far + dot(pres_hl[:, ahead], diff_l[ahead, cols])
            moved = vel_l[:, cols] - rows_l[6:7, cols] * (grad_l[:, cols] + halves(far))
            vel_l[:, cols] = moved
            put_pieces(second, chunk, moved)
            send(second, (2 * chunk, 2 * chunk + 1))

        for chunk in range(4):
            cols = slice(chunk * 256, chunk * 256 + 256)
            gradient = halves(dot(pres_hl[...], diff[:, cols]))
            moved = vel[:, cols] - rows_l[2:3, cols] * gradient
            vel[:, cols] = moved
            high, low = split(moved)
            vel_hl[:LP, cols] = high
            vel_hl[LP:, cols] = low

        @pl.when(s == 0)
        def _():
            build_weight()
            build_solver()

        @pl.when(s == NSUB - 1)
        def _():
            v_out[...] = vel[:L, :E]

        def divergence(places):
            wide = dot(vel_hl[:, places], weight[places, :])
            return halves(wide[:, :C] + wide[:, C:])

        right[...] = pres[...] - divergence(slice(0, EP))
        receive(second, (3, 4), vel_hl, EP)
        right[...] = right[...] - divergence(slice(EP + 3 * H, EP + 5 * H))
        receive_rest(second, vel_hl, EP)
        total = divergence(slice(EP, EP + 3 * H)) + divergence(slice(EP + 5 * H, EP + 8 * H))
        to_columns(right[...] - total, solve_in)
        solve()

        @pl.when(s < NSUB - 1)
        def _():
            pressure_pieces(second + 1, True)
            own_gradient()

        return carry

    lax.fori_loop(0, NSUB, substep, 0)
    p_out[...] = pres[:L, :]
    for exchange in range(2 * NSUB):
        each(range(8), lambda turn: copy(exchange, turn).wait_send())


def store(p, v, p_out, v_out, sem):
    copies = [
        pltpu.make_async_copy(p, p_out.at[:, 0, :], sem.at[0]),
        pltpu.make_async_copy(v, v_out.at[:, 0, :], sem.at[1]),
    ]
    for copy in copies:
        copy.start()
    for copy in copies:
        copy.wait()


def solution(mesh):
    n_lat, n_lon = mesh.shape["lat"], mesh.shape["lon"]
    any_space = pl.BlockSpec(memory_space=pl.ANY)
    vmem = pltpu.VMEM
    i32 = jnp.int32

    def turned(x):
        return jnp.transpose(x, (1, 0, 2))

    def on_device(p, v, ec, ce, sc, se, inv, w, ss, cp):
        results = pl.pallas_call(
            functools.partial(kernel, n_lat, n_lon),
            out_shape=(
                vmem((L, C), F32),
                vmem((L, E), F32),
            ),
            in_specs=[any_space] * 10,
            out_specs=(pl.BlockSpec(memory_space=vmem),) * 2,
            scratch_shapes=[
                vmem((L, C), F32), vmem((L, E), F32),
                vmem((2, E), i32), vmem((3, C), i32), vmem((8, H), i32), vmem((8, H), i32),
                vmem((1, E), F32), vmem((3, C), F32), vmem((1, C), F32), vmem((L, C), F32),
                vmem((LP, C), F32), vmem((LP, EP), F32),
                vmem((2 * NSUB, 8, L, H), F32), vmem((2 * NSUB, 8, L, H), F32),
                vmem((2 * LP, C + N), BF16), vmem((2 * LP, EP + N), BF16),
                vmem((C, N), BF16), vmem((EP, N), BF16),
                vmem((C + N, N), BF16), vmem((C + N, N), BF16), vmem((EP + N, 2 * C), BF16),
                vmem((8, N), F32), vmem((LP, N), F32), vmem((LP, N), F32), vmem((LP, C), F32),
                vmem((8 * LP, H), F32), vmem((8 * LP, H), F32),
                vmem((8 * LP, H), F32), vmem((8 * LP, H), F32), vmem((8 * LP, H), F32),
                pltpu.SemaphoreType.DMA((10,)),
                pltpu.SemaphoreType.DMA((2 * NSUB, 8)), pltpu.SemaphoreType.DMA((2 * NSUB, 8)),
            ],
            compiler_params=pltpu.CompilerParams(
                collective_id=0, has_side_effects=True, vmem_limit_bytes=60 * 1024 * 1024
            ),
        )(turned(p), turned(v), ec, turned(ce), sc, se, inv, turned(w), ss, turned(cp))
        stored = pl.pallas_call(
            store,
            out_shape=(
                jax.ShapeDtypeStruct((L, 1, C), F32),
                jax.ShapeDtypeStruct((L, 1, E), F32),
            ),
            in_specs=[pl.BlockSpec(memory_space=vmem)] * 2,
            out_specs=(any_space, any_space),
            scratch_shapes=[pltpu.SemaphoreType.DMA((2,))],
            compiler_params=pltpu.CompilerParams(vmem_limit_bytes=1024 * 1024),
        )(*results)
        return tuple(turned(x) for x in stored)

    spec3, spec2 = P("lat", None, "lon"), P("lat", "lon")
    return jax.shard_map(
        on_device,
        mesh=mesh,
        in_specs=(spec3, spec3, spec3, spec3, spec3, spec3, spec2, spec3, spec2, spec3),
        out_specs=(spec3, spec3),
        check_vma=False,
    )
```

```python
import functools

import jax
import jax.numpy as jnp
from jax import lax
from jax.experimental import pallas as pl
from jax.experimental.pallas import tpu as pltpu
from jax.sharding import PartitionSpec as P

NSUB = 3
C = 640
E = 960
EP = 1024
H = 128
L = 30
MID = L // 2
LP = 32
N = 8 * H
DIRECTIONS = ((-1, -1), (-1, 0), (-1, 1), (0, -1), (0, 1), (1, -1), (1, 0), (1, 1))
F32, BF16 = jnp.float32, jnp.bfloat16
MESH = pl.DeviceIdType.MESH


def split(x):
    high = x.astype(BF16)
    return high, (x - high.astype(F32)).astype(BF16)


def dot(a, b):
    return jnp.dot(a, b, preferred_element_type=F32)


def halves(x):
    return x[:LP] + x[LP:]


def kernel(
    n_lat, n_lon,
    p_hbm, v_hbm, ec_hbm, ce_hbm, sc_hbm, se_hbm, inv_hbm, w_hbm, ss_hbm, cp_hbm,
    p_out, v_out,
    p_in, v_in, ec_in, ce_in, sc_in, se_in, inv_in, w_in, ss_in, cp_in,
    pres, vel, pieces_out, pieces_in,
    pres_hl, vel_hl, pick_c, pick_e, diff, diff_l, weight,
    rows_l, grad_l, vel_l, right, solve_in, solve_mid, coef_a, coef_b, coef_r,
    in_sem, send_sem, recv_sem,
):
    a, b = lax.axis_index("lat"), lax.axis_index("lon")
    not_first, not_last = a > 0, a < n_lat - 1

    def device_at(p, q):
        return (a + p, lax.rem(b + q + n_lon, n_lon))

    def neighbour(member):
        return device_at(*DIRECTIONS[member])

    core = lax.rem(b, 2)
    cross = 2 * core - 1
    order = (
        (-1, cross, 2 * core), (1, cross, 5 + 2 * core),
        (-1, -cross, 2 - 2 * core), (1, -cross, 7 - 2 * core),
        (-1, 0, 1), (1, 0, 6), (0, cross, 3 + core), (0, -cross, 4 - core),
    )

    sources = (sc_hbm, p_hbm, se_hbm, v_hbm, ec_hbm, inv_hbm, ce_hbm, w_hbm, ss_hbm, cp_hbm)
    targets = (sc_in, p_in, se_in, v_in, ec_in, inv_in, ce_in, w_in, ss_in, cp_in)
    loads = []
    for i, (source, target) in enumerate(zip(sources, targets)):
        if source.ndim == 2:
            view = source
        else:
            view = source.at[0] if source.shape[0] == 1 else source.at[:, 0, :]
        loads.append(pltpu.make_async_copy(view, target, in_sem.at[i]))
    loads[0].start()
    loads[1].start()

    barrier = pltpu.get_barrier_semaphore()

    def greet(members):
        for member in members:
            pl.semaphore_signal(barrier, inc=1, device_id=neighbour(member), device_id_type=MESH)

    greet((3, 4))
    pl.when(not_first)(lambda: greet((0, 1, 2)))
    pl.when(not_last)(lambda: greet((5, 6, 7)))

    for load in loads[2:]:
        load.start()

    def copy(exchange, turn):
        p, q, member = order[turn]
        return pltpu.make_async_remote_copy(
            src_ref=pieces_out.at[exchange, turn],
            dst_ref=pieces_in.at[exchange, 7 - member],
            send_sem=send_sem.at[exchange, turn],
            recv_sem=recv_sem.at[exchange, 7 - member],
            device_id=device_at(p, q),
            device_id_type=MESH,
        )

    def each(turns, action):
        for turn in turns:
            row = order[turn][0]
            if row == 0:
                action(turn)
            else:
                pl.when(not_first if row < 0 else not_last)(functools.partial(action, turn))

    def send(exchange, turns):
        each(turns, lambda turn: copy(exchange, turn).start())

    def receive(exchange, first, count, target, base):
        for i in range(count):
            pltpu.make_async_remote_copy(
                src_ref=pieces_out.at[exchange, i],
                dst_ref=pieces_in.at[exchange, first + i],
                send_sem=send_sem.at[exchange, i],
                recv_sem=recv_sem.at[exchange, first + i],
                device_id=device_at(0, 1),
                device_id_type=MESH,
            ).wait_recv()
        for i in range(count):
            high, low = split(pieces_in[exchange, first + i])
            cols = pl.ds(pl.multiple_of(base + (first + i) * H, H), H)
            target[:L, cols] = high
            target[LP:LP + L, cols] = low

    ahead_first = 1 - lax.min(lax.rem(a, 4), 1)
    groups = (
        (5 * ahead_first, jnp.where(ahead_first == 1, not_last, not_first)),
        (5 - 5 * ahead_first, jnp.where(ahead_first == 1, not_first, not_last)),
    )

    def receive_group(exchange, group, target, base):
        first, there = groups[group]
        pl.when(there)(lambda: receive(exchange, first, 3, target, base))

    def group_places(group, base):
        return pl.ds(pl.multiple_of(base + groups[group][0] * H, H), 3 * H)

    def in_blocks(count, build):
        def step(block, carry):
            start = pl.multiple_of(block * H, H)
            base = start.astype(F32)

            def local(places):
                within = places - base
                within = jnp.where((within >= 0.0) & (within < float(H)), within, -1.0)
                return jnp.broadcast_to(within, (16, places.shape[1])).astype(BF16)

            build(start, local)
            return carry

        lax.fori_loop(0, count // H, step, 0)

    def row_numbers(j, width):
        return (lax.broadcasted_iota(jnp.int32, (16, width), 0) + 16 * j).astype(F32).astype(BF16)

    def build_pick(lists_ref, target, own):
        lists = lists_ref[...].astype(F32)

        def either(first, second):
            return jnp.where(core == 0, lists[first:first + 1], lists[second:second + 1])

        picks = jnp.concatenate(
            [either(0, 2), either(5, 7), either(2, 0), either(7, 5),
             lists[1:2], lists[6:7], either(3, 4), either(4, 3)], axis=1)

        def build(start, local):
            here = local(picks)
            one, zero = jnp.ones((16, N), BF16), jnp.zeros((16, N), BF16)
            for j in range(H // 16):
                target[pl.ds(start + 16 * j, 16), :] = jnp.where(row_numbers(j, N) == here, one, zero)

        in_blocks(own, build)

    def build_diff(first, second, target):
        def build(start, local):
            minus, plus = local(first), local(second)
            one, zero = jnp.ones((16, N), BF16), jnp.zeros((16, N), BF16)
            for j in range(H // 16):
                rows = row_numbers(j, N)
                hit = jnp.where(rows == plus, one, zero) - jnp.where(rows == minus, one, zero)
                target[pl.ds(start + 16 * j, 16), :] = hit

        in_blocks(C + N, build)

    def build_weight():
        places = ce_in[...].astype(F32)
        places = jnp.where(places >= E, places + (EP - E), places)
        weights = w_in[...] * ss_in[...]
        place = [places[j:j + 1] for j in range(3)]
        factor = [weights[j:j + 1] for j in range(3)]
        for i, j in ((0, 1), (0, 2), (1, 2)):
            same = place[i] == place[j]
            factor[i] = factor[i] + jnp.where(same, factor[j], 0.0)
            place[j] = jnp.where(same, -1.0, place[j])
        parts = [split(jnp.broadcast_to(x, (16, C))) for x in factor]

        def build(start, local):
            here = [local(x) for x in place]
            zero = jnp.zeros((16, C), BF16)
            for j in range(H // 16):
                rows = row_numbers(j, C)
                high, low = zero, zero
                for where, (part_high, part_low) in zip(here, parts):
                    hit = rows == where
                    high, low = jnp.where(hit, part_high, high), jnp.where(hit, part_low, low)
                weight[pl.ds(start + 16 * j, 16), :C] = high
                weight[pl.ds(start + 16 * j, 16), C:] = low

        in_blocks(EP + N, build)

    def to_columns(x, target):
        for block in range(C // H):
            target[pl.ds(block, LP, stride=8), :] = x[:, block * H:(block + 1) * H]

    def build_solver():
        coupling = jnp.concatenate([cp_in[...], jnp.zeros((LP - L, C), F32)], axis=0)
        to_columns(coupling, solve_in)

        def rows(k):
            return slice(8 * k, 8 * k + 8)

        inverse = None
        for k in range(MID):
            above = solve_in[rows(k), :]
            divisor = 1.0 + above
            if k > 0:
                below = solve_in[rows(k - 1), :]
                divisor = divisor + below - below * (below * inverse)
            inverse = 1.0 / divisor
            coef_a[rows(k), :] = inverse
            if k > 0:
                coef_b[rows(k), :] = below * inverse
            coef_r[rows(k), :] = above * inverse
        inverse = None
        for k in range(L - 1, MID - 1, -1):
            above, below = solve_in[rows(k), :], solve_in[rows(k - 1), :]
            divisor = 1.0 + above + below
            if k < L - 1:
                divisor = divisor - above * (above * inverse)
            inverse = 1.0 / divisor
            coef_a[rows(k), :] = inverse
            if k < L - 1:
                coef_b[rows(k), :] = above * inverse
            coef_r[rows(k), :] = below * inverse
        coef_b[rows(0), :] = 1.0 / (1.0 - coef_r[rows(MID - 1), :] * coef_r[rows(MID), :])

    def solve():
        def rows(k):
            return slice(8 * k, 8 * k + 8)

        low = solve_in[rows(0), :] * coef_a[rows(0), :]
        high = solve_in[rows(L - 1), :] * coef_a[rows(L - 1), :]
        solve_mid[rows(0), :] = low
        solve_mid[rows(L - 1), :] = high
        for k in range(1, MID):
            up, down = rows(k), rows(L - 1 - k)
            low = solve_in[up, :] * coef_a[up, :] + coef_b[up, :] * low
            high = solve_in[down, :] * coef_a[down, :] + coef_b[down, :] * high
            if k < MID - 1:
                solve_mid[up, :] = low
                solve_mid[down, :] = high
        meet = coef_b[rows(0), :]
        low, high = (
            (low + coef_r[rows(MID - 1), :] * high) * meet,
            (high + coef_r[rows(MID), :] * low) * meet,
        )
        solve_mid[rows(MID - 1), :] = low
        solve_mid[rows(MID), :] = high
        for k in range(MID - 2, -1, -1):
            up, down = rows(k), rows(L - 1 - k)
            low = solve_mid[up, :] + coef_r[up, :] * low
            high = solve_mid[down, :] + coef_r[down, :] * high
            solve_mid[up, :] = low
            solve_mid[down, :] = high
        for block in range(C // H):
            x = solve_mid[pl.ds(block, LP, stride=8), :]
            pres[:, block * H:(block + 1) * H] = x
            high, low = split(x)
            pres_hl[:LP, block * H:(block + 1) * H] = high
            pres_hl[LP:, block * H:(block + 1) * H] = low

    def put_pieces(exchange, chunk, x):
        for half in range(2):
            pieces_out[exchange, 2 * chunk + half] = x[:L, half * H:(half + 1) * H]

    def pressure_pieces(exchange):
        for chunk in range(4):
            cols = slice(chunk * 256, chunk * 256 + 256)
            put_pieces(exchange, chunk, halves(dot(pres_hl[:, :C], pick_c[:, cols])))
            send(exchange, (2 * chunk, 2 * chunk + 1))

    def own_gradient():
        for chunk in range(4):
            cols = slice(chunk * 256, chunk * 256 + 256)
            grad_l[:, cols] = halves(dot(pres_hl[:, :C], diff_l[:C, cols]))

    loads[0].wait()
    build_pick(sc_in, pick_c, C)
    loads[1].wait()
    start = jnp.concatenate([p_in[...], jnp.zeros((LP - L, C), F32)], axis=0)
    pres[...] = start
    high, low = split(start)
    pres_hl[:LP, :C] = high
    pres_hl[LP:, :C] = low
    pres_hl[:, C:] = jnp.zeros((2 * LP, N), BF16)
    pl.semaphore_wait(barrier, 2 + 3 * lax.min(a, 1) + 3 * lax.min(n_lat - 1 - a, 1))
    pressure_pieces(0)

    loads[2].wait()
    build_pick(se_in, pick_e, EP)
    for i in range(3, 10):
        loads[i].wait()
    vel[...] = jnp.zeros_like(vel)
    vel[:L, :E] = v_in[...]
    high, low = split(vel[...])
    vel_hl[:LP, :EP] = high
    vel_hl[LP:, :EP] = low
    vel_hl[:, EP:] = jnp.zeros((2 * LP, N), BF16)
    rows_l[...] = jnp.full(rows_l.shape, -1.0, F32)
    rows_l[0:2, :E] = ec_in[...].astype(F32)
    rows_l[2:3, :] = jnp.zeros((1, EP), F32)
    rows_l[2:3, :E] = 0.5 * inv_in[...]
    own_rows = rows_l[...]
    cells_first, cells_second, factor = own_rows[0:1], own_rows[1:2], own_rows[2:3]
    coarse = jnp.floor(own_rows[0:2] * (1.0 / H))
    fine = own_rows[0:2] - H * coarse
    factor_high = factor.astype(BF16).astype(F32)
    factor_mid = (factor - factor_high).astype(BF16).astype(F32)
    factor_low = factor - factor_high - factor_mid
    parts = jnp.concatenate(
        [coarse, fine, factor_high, factor_mid, factor_low, jnp.zeros((9, EP), F32)], axis=0
    ).astype(BF16)
    for chunk in range(4):
        cols = slice(chunk * 256, chunk * 256 + 256)
        vel_l[:, cols] = halves(dot(vel_hl[:, :EP], pick_e[:, cols]))
        found = dot(parts, pick_e[:, cols])
        rows_l[4:6, cols] = found[0:2] * H + found[2:4]
        rows_l[6:7, cols] = found[4:5] + found[5:6] + found[6:7]
    sent_rows = rows_l[...]
    build_diff(sent_rows[4:5], sent_rows[5:6], diff_l)
    own_gradient()
    build_diff(cells_first, cells_second, diff)

    def substep(s, carry):
        first, second = 2 * s, 2 * s + 1
        def add_gradient(places):
            for chunk in range(4):
                cols = slice(chunk * 256, chunk * 256 + 256)
                grad_l[:, cols] = grad_l[:, cols] + halves(dot(pres_hl[:, places], diff_l[places, cols]))

        receive(first, 3, 2, pres_hl, C)
        add_gradient(slice(C + 3 * H, C + 5 * H))
        receive_group(first, 0, pres_hl, C)
        add_gradient(group_places(0, C))
        receive_group(first, 1, pres_hl, C)
        places = group_places(1, C)
        for chunk in range(4):
            cols = slice(chunk * 256, chunk * 256 + 256)
            gradient = grad_l[:, cols] + halves(dot(pres_hl[:, places], diff_l[places, cols]))
            moved = vel_l[:, cols] - rows_l[6:7, cols] * gradient
            vel_l[:, cols] = moved
            put_pieces(second, chunk, moved)
            send(second, (2 * chunk, 2 * chunk + 1))

        for chunk in range(4):
            cols = slice(chunk * 256, chunk * 256 + 256)
            gradient = halves(dot(pres_hl[...], diff[:, cols]))
            moved = vel[:, cols] - rows_l[2:3, cols] * gradient
            vel[:, cols] = moved
            high, low = split(moved)
            vel_hl[:LP, cols] = high
            vel_hl[LP:, cols] = low

        @pl.when(s == 0)
        def _():
            build_weight()
            build_solver()

        @pl.when(s == NSUB - 1)
        def _():
            v_out[...] = vel[:L, :E]

        def divergence(places):
            wide = dot(vel_hl[:, places], weight[places, :])
            return halves(wide[:, :C] + wide[:, C:])

        right[...] = pres[...] - divergence(slice(0, EP))
        receive(second, 3, 2, vel_hl, EP)
        right[...] = right[...] - divergence(slice(EP + 3 * H, EP + 5 * H))
        receive_group(second, 0, vel_hl, EP)
        right[...] = right[...] - divergence(group_places(0, EP))
        receive_group(second, 1, vel_hl, EP)
        to_columns(right[...] - divergence(group_places(1, EP)), solve_in)
        solve()

        @pl.when(s < NSUB - 1)
        def _():
            pressure_pieces(second + 1)
            own_gradient()

        return carry

    lax.fori_loop(0, NSUB, substep, 0)
    p_out[...] = pres[:L, :]
    for exchange in range(2 * NSUB):
        each(range(8), lambda turn: copy(exchange, turn).wait_send())


def store(p, v, p_out, v_out, sem):
    copies = [
        pltpu.make_async_copy(p, p_out.at[:, 0, :], sem.at[0]),
        pltpu.make_async_copy(v, v_out.at[:, 0, :], sem.at[1]),
    ]
    for copy in copies:
        copy.start()
    for copy in copies:
        copy.wait()


def solution(mesh):
    n_lat, n_lon = mesh.shape["lat"], mesh.shape["lon"]
    any_space = pl.BlockSpec(memory_space=pl.ANY)
    vmem = pltpu.VMEM
    i32 = jnp.int32

    def turned(x):
        return jnp.transpose(x, (1, 0, 2))

    def on_device(p, v, ec, ce, sc, se, inv, w, ss, cp):
        results = pl.pallas_call(
            functools.partial(kernel, n_lat, n_lon),
            out_shape=(
                vmem((L, C), F32),
                vmem((L, E), F32),
            ),
            in_specs=[any_space] * 10,
            out_specs=(pl.BlockSpec(memory_space=vmem),) * 2,
            scratch_shapes=[
                vmem((L, C), F32), vmem((L, E), F32),
                vmem((2, E), i32), vmem((3, C), i32), vmem((8, H), i32), vmem((8, H), i32),
                vmem((1, E), F32), vmem((3, C), F32), vmem((1, C), F32), vmem((L, C), F32),
                vmem((LP, C), F32), vmem((LP, EP), F32),
                vmem((2 * NSUB, 8, L, H), F32), vmem((2 * NSUB, 8, L, H), F32),
                vmem((2 * LP, C + N), BF16), vmem((2 * LP, EP + N), BF16),
                vmem((C, N), BF16), vmem((EP, N), BF16),
                vmem((C + N, N), BF16), vmem((C + N, N), BF16), vmem((EP + N, 2 * C), BF16),
                vmem((8, N), F32), vmem((LP, N), F32), vmem((LP, N), F32), vmem((LP, C), F32),
                vmem((8 * LP, H), F32), vmem((8 * LP, H), F32),
                vmem((8 * LP, H), F32), vmem((8 * LP, H), F32), vmem((8 * LP, H), F32),
                pltpu.SemaphoreType.DMA((10,)),
                pltpu.SemaphoreType.DMA((2 * NSUB, 8)), pltpu.SemaphoreType.DMA((2 * NSUB, 8)),
            ],
            compiler_params=pltpu.CompilerParams(
                collective_id=0, has_side_effects=True, vmem_limit_bytes=60 * 1024 * 1024
            ),
        )(turned(p), turned(v), ec, turned(ce), sc, se, inv, turned(w), ss, turned(cp))
        stored = pl.pallas_call(
            store,
            out_shape=(
                jax.ShapeDtypeStruct((L, 1, C), F32),
                jax.ShapeDtypeStruct((L, 1, E), F32),
            ),
            in_specs=[pl.BlockSpec(memory_space=vmem)] * 2,
            out_specs=(any_space, any_space),
            scratch_shapes=[pltpu.SemaphoreType.DMA((2,))],
            compiler_params=pltpu.CompilerParams(vmem_limit_bytes=1024 * 1024),
        )(*results)
        return tuple(turned(x) for x in stored)

    spec3, spec2 = P("lat", None, "lon"), P("lat", "lon")
    return jax.shard_map(
        on_device,
        mesh=mesh,
        in_specs=(spec3, spec3, spec3, spec3, spec3, spec3, spec2, spec3, spec2, spec3),
        out_specs=(spec3, spec3),
        check_vma=False,
    )
```

```python
import functools

import jax
import jax.numpy as jnp
from jax import lax
from jax.experimental import pallas as pl
from jax.experimental.pallas import tpu as pltpu
from jax.sharding import PartitionSpec as P

NSUB = 3
C = 640
E = 960
EP = 1024
H = 128
L = 30
MID = L // 2
LP = 32
N = 8 * H
DIRECTIONS = ((-1, -1), (-1, 0), (-1, 1), (0, -1), (0, 1), (1, -1), (1, 0), (1, 1))
F32, BF16 = jnp.float32, jnp.bfloat16
MESH = pl.DeviceIdType.MESH


def split(x):
    high = x.astype(BF16)
    return high, (x - high.astype(F32)).astype(BF16)


def dot(a, b):
    return jnp.dot(a, b, preferred_element_type=F32)


def halves(x):
    return x[:LP] + x[LP:]


def kernel(
    n_lat, n_lon,
    p_hbm, v_hbm, ec_hbm, ce_hbm, sc_hbm, se_hbm, inv_hbm, w_hbm, ss_hbm, cp_hbm,
    p_out, v_out,
    p_in, v_in, ec_in, ce_in, sc_in, se_in, inv_in, w_in, ss_in, cp_in,
    pres, vel, pieces_out, pieces_in,
    pres_hl, vel_hl, pick_c, pick_e, diff, diff_l, weight,
    rows_l, grad_l, vel_l, right, solve_in, solve_mid, coef_a, coef_b, coef_r,
    in_sem, send_sem, recv_sem,
):
    a, b = lax.axis_index("lat"), lax.axis_index("lon")
    not_first, not_last = a > 0, a < n_lat - 1

    def device_at(p, q):
        return (a + p, lax.rem(b + q + n_lon, n_lon))

    def neighbour(member):
        return device_at(*DIRECTIONS[member])

    core = lax.rem(b, 2)
    cross = 2 * core - 1
    order = (
        (-1, cross, 2 * core), (1, cross, 5 + 2 * core),
        (-1, -cross, 2 - 2 * core), (1, -cross, 7 - 2 * core),
        (-1, 0, 1), (1, 0, 6), (0, cross, 3 + core), (0, -cross, 4 - core),
    )

    sources = (sc_hbm, p_hbm, se_hbm, v_hbm, ec_hbm, inv_hbm, ce_hbm, w_hbm, ss_hbm, cp_hbm)
    targets = (sc_in, p_in, se_in, v_in, ec_in, inv_in, ce_in, w_in, ss_in, cp_in)
    loads = []
    for i, (source, target) in enumerate(zip(sources, targets)):
        if source.ndim == 2:
            view = source
        else:
            view = source.at[0] if source.shape[0] == 1 else source.at[:, 0, :]
        loads.append(pltpu.make_async_copy(view, target, in_sem.at[i]))
    loads[0].start()
    loads[1].start()

    barrier = pltpu.get_barrier_semaphore()

    def greet(members):
        for member in members:
            pl.semaphore_signal(barrier, inc=1, device_id=neighbour(member), device_id_type=MESH)

    greet((3, 4))
    pl.when(not_first)(lambda: greet((0, 1, 2)))
    pl.when(not_last)(lambda: greet((5, 6, 7)))

    for load in loads[2:]:
        load.start()

    def copy(exchange, turn):
        p, q, member = order[turn]
        return pltpu.make_async_remote_copy(
            src_ref=pieces_out.at[exchange, turn],
            dst_ref=pieces_in.at[exchange, 7 - member],
            send_sem=send_sem.at[exchange, turn],
            recv_sem=recv_sem.at[exchange, 7 - member],
            device_id=device_at(p, q),
            device_id_type=MESH,
        )

    def each(turns, action):
        for turn in turns:
            row = order[turn][0]
            if row == 0:
                action(turn)
            else:
                pl.when(not_first if row < 0 else not_last)(functools.partial(action, turn))

    def send(exchange, turns):
        each(turns, lambda turn: copy(exchange, turn).start())

    def receive(exchange, first, count, target, base):
        for i in range(count):
            pltpu.make_async_remote_copy(
                src_ref=pieces_out.at[exchange, i],
                dst_ref=pieces_in.at[exchange, first + i],
                send_sem=send_sem.at[exchange, i],
                recv_sem=recv_sem.at[exchange, first + i],
                device_id=device_at(0, 1),
                device_id_type=MESH,
            ).wait_recv()
        for i in range(count):
            high, low = split(pieces_in[exchange, first + i])
            cols = pl.ds(pl.multiple_of(base + (first + i) * H, H), H)
            target[:L, cols] = high
            target[LP:LP + L, cols] = low

    ahead_first = 1 - lax.min(lax.rem(a, 4), 1)
    groups = (
        (5 * ahead_first, jnp.where(ahead_first == 1, not_last, not_first)),
        (5 - 5 * ahead_first, jnp.where(ahead_first == 1, not_first, not_last)),
    )

    def receive_group(exchange, group, target, base):
        first, there = groups[group]
        pl.when(there)(lambda: receive(exchange, first, 3, target, base))

    def group_places(group, base):
        return pl.ds(pl.multiple_of(base + groups[group][0] * H, H), 3 * H)

    def in_blocks(count, build):
        def step(block, carry):
            start = pl.multiple_of(block * H, H)
            base = start.astype(F32)

            def local(places):
                within = places - base
                within = jnp.where((within >= 0.0) & (within < float(H)), within, -1.0)
                return jnp.broadcast_to(within, (16, places.shape[1])).astype(BF16)

            build(start, local)
            return carry

        lax.fori_loop(0, count // H, step, 0)

    def row_numbers(j, width):
        return (lax.broadcasted_iota(jnp.int32, (16, width), 0) + 16 * j).astype(F32).astype(BF16)

    def build_pick(lists_ref, target, own):
        lists = lists_ref[...].astype(F32)

        def either(first, second):
            return jnp.where(core == 0, lists[first:first + 1], lists[second:second + 1])

        picks = jnp.concatenate(
            [either(0, 2), either(5, 7), either(2, 0), either(7, 5),
             lists[1:2], lists[6:7], either(3, 4), either(4, 3)], axis=1)

        def build(start, local):
            here = local(picks)
            one, zero = jnp.ones((16, N), BF16), jnp.zeros((16, N), BF16)
            for j in range(H // 16):
                target[pl.ds(start + 16 * j, 16), :] = jnp.where(row_numbers(j, N) == here, one, zero)

        in_blocks(own, build)

    def build_diff(first, second, target):
        def build(start, local):
            minus, plus = local(first), local(second)
            one, zero = jnp.ones((16, N), BF16), jnp.zeros((16, N), BF16)
            for j in range(H // 16):
                rows = row_numbers(j, N)
                hit = jnp.where(rows == plus, one, zero) - jnp.where(rows == minus, one, zero)
                target[pl.ds(start + 16 * j, 16), :] = hit

        in_blocks(C + N, build)

    def build_weight():
        places = ce_in[...].astype(F32)
        places = jnp.where(places >= E, places + (EP - E), places)
        weights = w_in[...] * ss_in[...]
        place = [places[j:j + 1] for j in range(3)]
        factor = [weights[j:j + 1] for j in range(3)]
        for i, j in ((0, 1), (0, 2), (1, 2)):
            same = place[i] == place[j]
            factor[i] = factor[i] + jnp.where(same, factor[j], 0.0)
            place[j] = jnp.where(same, -1.0, place[j])
        parts = [split(jnp.broadcast_to(x, (16, C))) for x in factor]

        def build(start, local):
            here = [local(x) for x in place]
            zero = jnp.zeros((16, C), BF16)
            for j in range(H // 16):
                rows = row_numbers(j, C)
                high, low = zero, zero
                for where, (part_high, part_low) in zip(here, parts):
                    hit = rows == where
                    high, low = jnp.where(hit, part_high, high), jnp.where(hit, part_low, low)
                weight[pl.ds(start + 16 * j, 16), :C] = high
                weight[pl.ds(start + 16 * j, 16), C:] = low

        in_blocks(EP + N, build)

    def to_columns(x, target):
        for block in range(C // H):
            target[pl.ds(block, LP, stride=8), :] = x[:, block * H:(block + 1) * H]

    def build_solver():
        coupling = jnp.concatenate([cp_in[...], jnp.zeros((LP - L, C), F32)], axis=0)
        to_columns(coupling, solve_in)

        def rows(k):
            return slice(8 * k, 8 * k + 8)

        inverse = None
        for k in range(MID):
            above = solve_in[rows(k), :]
            divisor = 1.0 + above
            if k > 0:
                below = solve_in[rows(k - 1), :]
                divisor = divisor + below - below * (below * inverse)
            inverse = 1.0 / divisor
            coef_a[rows(k), :] = inverse
            if k > 0:
                coef_b[rows(k), :] = below * inverse
            coef_r[rows(k), :] = above * inverse
        inverse = None
        for k in range(L - 1, MID - 1, -1):
            above, below = solve_in[rows(k), :], solve_in[rows(k - 1), :]
            divisor = 1.0 + above + below
            if k < L - 1:
                divisor = divisor - above * (above * inverse)
            inverse = 1.0 / divisor
            coef_a[rows(k), :] = inverse
            if k < L - 1:
                coef_b[rows(k), :] = above * inverse
            coef_r[rows(k), :] = below * inverse
        coef_b[rows(0), :] = 1.0 / (1.0 - coef_r[rows(MID - 1), :] * coef_r[rows(MID), :])

    def solve():
        def rows(k):
            return slice(8 * k, 8 * k + 8)

        low = solve_in[rows(0), :] * coef_a[rows(0), :]
        high = solve_in[rows(L - 1), :] * coef_a[rows(L - 1), :]
        solve_mid[rows(0), :] = low
        solve_mid[rows(L - 1), :] = high
        for k in range(1, MID):
            up, down = rows(k), rows(L - 1 - k)
            low = solve_in[up, :] * coef_a[up, :] + coef_b[up, :] * low
            high = solve_in[down, :] * coef_a[down, :] + coef_b[down, :] * high
            if k < MID - 1:
                solve_mid[up, :] = low
                solve_mid[down, :] = high
        meet = coef_b[rows(0), :]
        low, high = (
            (low + coef_r[rows(MID - 1), :] * high) * meet,
            (high + coef_r[rows(MID), :] * low) * meet,
        )
        solve_mid[rows(MID - 1), :] = low
        solve_mid[rows(MID), :] = high
        for k in range(MID - 2, -1, -1):
            up, down = rows(k), rows(L - 1 - k)
            low = solve_mid[up, :] + coef_r[up, :] * low
            high = solve_mid[down, :] + coef_r[down, :] * high
            solve_mid[up, :] = low
            solve_mid[down, :] = high
        for block in range(C // H):
            x = solve_mid[pl.ds(block, LP, stride=8), :]
            pres[:, block * H:(block + 1) * H] = x
            high, low = split(x)
            pres_hl[:LP, block * H:(block + 1) * H] = high
            pres_hl[LP:, block * H:(block + 1) * H] = low

    def put_and_send(exchange, chunks):
        for chunk, x in enumerate(chunks):
            for half in range(2):
                pieces_out[exchange, 2 * chunk + half] = x[:L, half * H:(half + 1) * H]
            send(exchange, (2 * chunk, 2 * chunk + 1))

    def pressure_pieces(exchange):
        products = [dot(pres_hl[:, :C], pick_c[:, chunk * 256:chunk * 256 + 256]) for chunk in range(4)]
        put_and_send(exchange, [halves(x) for x in products])

    def own_gradient():
        for chunk in range(4):
            cols = slice(chunk * 256, chunk * 256 + 256)
            grad_l[:, cols] = halves(dot(pres_hl[:, :C], diff_l[:C, cols]))

    loads[0].wait()
    build_pick(sc_in, pick_c, C)
    loads[1].wait()
    start = jnp.concatenate([p_in[...], jnp.zeros((LP - L, C), F32)], axis=0)
    pres[...] = start
    high, low = split(start)
    pres_hl[:LP, :C] = high
    pres_hl[LP:, :C] = low
    pres_hl[:, C:] = jnp.zeros((2 * LP, N), BF16)
    pl.semaphore_wait(barrier, 2 + 3 * lax.min(a, 1) + 3 * lax.min(n_lat - 1 - a, 1))
    pressure_pieces(0)

    loads[2].wait()
    build_pick(se_in, pick_e, EP)
    for i in range(3, 10):
        loads[i].wait()
    vel[...] = jnp.zeros_like(vel)
    vel[:L, :E] = v_in[...]
    high, low = split(vel[...])
    vel_hl[:LP, :EP] = high
    vel_hl[LP:, :EP] = low
    vel_hl[:, EP:] = jnp.zeros((2 * LP, N), BF16)
    rows_l[...] = jnp.full(rows_l.shape, -1.0, F32)
    rows_l[0:2, :E] = ec_in[...].astype(F32)
    rows_l[2:3, :] = jnp.zeros((1, EP), F32)
    rows_l[2:3, :E] = 0.5 * inv_in[...]
    own_rows = rows_l[...]
    cells_first, cells_second, factor = own_rows[0:1], own_rows[1:2], own_rows[2:3]
    coarse = jnp.floor(own_rows[0:2] * (1.0 / H))
    fine = own_rows[0:2] - H * coarse
    factor_high = factor.astype(BF16).astype(F32)
    factor_mid = (factor - factor_high).astype(BF16).astype(F32)
    factor_low = factor - factor_high - factor_mid
    parts = jnp.concatenate(
        [coarse, fine, factor_high, factor_mid, factor_low, jnp.zeros((9, EP), F32)], axis=0
    ).astype(BF16)
    for chunk in range(4):
        cols = slice(chunk * 256, chunk * 256 + 256)
        vel_l[:, cols] = halves(dot(vel_hl[:, :EP], pick_e[:, cols]))
        found = dot(parts, pick_e[:, cols])
        rows_l[4:6, cols] = found[0:2] * H + found[2:4]
        rows_l[6:7, cols] = found[4:5] + found[5:6] + found[6:7]
    sent_rows = rows_l[...]
    build_diff(sent_rows[4:5], sent_rows[5:6], diff_l)
    own_gradient()
    build_diff(cells_first, cells_second, diff)

    def substep(s, carry):
        first, second = 2 * s, 2 * s + 1
        receive(first, 3, 2, pres_hl, C)
        receive_group(first, 0, pres_hl, C)
        near, places = slice(C + 3 * H, C + 5 * H), group_places(0, C)
        for chunk in range(4):
            cols = slice(chunk * 256, chunk * 256 + 256)
            sums = dot(pres_hl[:, near], diff_l[near, cols]) + dot(pres_hl[:, places], diff_l[places, cols])
            grad_l[:, cols] = grad_l[:, cols] + halves(sums)
        receive_group(first, 1, pres_hl, C)
        places = group_places(1, C)
        products = [dot(pres_hl[:, places], diff_l[places, chunk * 256:chunk * 256 + 256]) for chunk in range(4)]
        moved = []
        for chunk in range(4):
            cols = slice(chunk * 256, chunk * 256 + 256)
            gradient = grad_l[:, cols] + halves(products[chunk])
            moved.append(vel_l[:, cols] - rows_l[6:7, cols] * gradient)
        put_and_send(second, moved)
        for chunk in range(4):
            vel_l[:, chunk * 256:chunk * 256 + 256] = moved[chunk]

        for chunk in range(4):
            cols = slice(chunk * 256, chunk * 256 + 256)
            gradient = halves(dot(pres_hl[...], diff[:, cols]))
            moved = vel[:, cols] - rows_l[2:3, cols] * gradient
            vel[:, cols] = moved
            high, low = split(moved)
            vel_hl[:LP, cols] = high
            vel_hl[LP:, cols] = low

        @pl.when(s == 0)
        def _():
            build_weight()
            build_solver()

        @pl.when(s == NSUB - 1)
        def _():
            v_out[...] = vel[:L, :E]

        def divergence(*ranges):
            wide = sum(dot(vel_hl[:, places], weight[places, :]) for places in ranges)
            return halves(wide[:, :C] + wide[:, C:])

        right[...] = pres[...] - divergence(slice(0, EP))
        each(range(8), lambda turn: copy(first, turn).wait_send())
        each(range(8), lambda turn: copy(second, turn).wait_send())
        receive(second, 3, 2, vel_hl, EP)
        receive_group(second, 0, vel_hl, EP)
        right[...] = right[...] - divergence(slice(EP + 3 * H, EP + 5 * H), group_places(0, EP))
        receive_group(second, 1, vel_hl, EP)
        to_columns(right[...] - divergence(group_places(1, EP)), solve_in)
        solve()

        @pl.when(s < NSUB - 1)
        def _():
            pressure_pieces(second + 1)
            own_gradient()

        return carry

    lax.fori_loop(0, NSUB, substep, 0)
    p_out[...] = pres[:L, :]


def store(p, v, p_out, v_out, sem):
    copies = [
        pltpu.make_async_copy(p, p_out.at[:, 0, :], sem.at[0]),
        pltpu.make_async_copy(v, v_out.at[:, 0, :], sem.at[1]),
    ]
    for copy in copies:
        copy.start()
    for copy in copies:
        copy.wait()


def solution(mesh):
    n_lat, n_lon = mesh.shape["lat"], mesh.shape["lon"]
    any_space = pl.BlockSpec(memory_space=pl.ANY)
    vmem = pltpu.VMEM
    i32 = jnp.int32

    def turned(x):
        return jnp.transpose(x, (1, 0, 2))

    def on_device(p, v, ec, ce, sc, se, inv, w, ss, cp):
        results = pl.pallas_call(
            functools.partial(kernel, n_lat, n_lon),
            out_shape=(
                vmem((L, C), F32),
                vmem((L, E), F32),
            ),
            in_specs=[any_space] * 10,
            out_specs=(pl.BlockSpec(memory_space=vmem),) * 2,
            scratch_shapes=[
                vmem((L, C), F32), vmem((L, E), F32),
                vmem((2, E), i32), vmem((3, C), i32), vmem((8, H), i32), vmem((8, H), i32),
                vmem((1, E), F32), vmem((3, C), F32), vmem((1, C), F32), vmem((L, C), F32),
                vmem((LP, C), F32), vmem((LP, EP), F32),
                vmem((2 * NSUB, 8, L, H), F32), vmem((2 * NSUB, 8, L, H), F32),
                vmem((2 * LP, C + N), BF16), vmem((2 * LP, EP + N), BF16),
                vmem((C, N), BF16), vmem((EP, N), BF16),
                vmem((C + N, N), BF16), vmem((C + N, N), BF16), vmem((EP + N, 2 * C), BF16),
                vmem((8, N), F32), vmem((LP, N), F32), vmem((LP, N), F32), vmem((LP, C), F32),
                vmem((8 * LP, H), F32), vmem((8 * LP, H), F32),
                vmem((8 * LP, H), F32), vmem((8 * LP, H), F32), vmem((8 * LP, H), F32),
                pltpu.SemaphoreType.DMA((10,)),
                pltpu.SemaphoreType.DMA((2 * NSUB, 8)), pltpu.SemaphoreType.DMA((2 * NSUB, 8)),
            ],
            compiler_params=pltpu.CompilerParams(
                collective_id=0, has_side_effects=True, vmem_limit_bytes=60 * 1024 * 1024
            ),
        )(turned(p), turned(v), ec, turned(ce), sc, se, inv, turned(w), ss, turned(cp))
        stored = pl.pallas_call(
            store,
            out_shape=(
                jax.ShapeDtypeStruct((L, 1, C), F32),
                jax.ShapeDtypeStruct((L, 1, E), F32),
            ),
            in_specs=[pl.BlockSpec(memory_space=vmem)] * 2,
            out_specs=(any_space, any_space),
            scratch_shapes=[pltpu.SemaphoreType.DMA((2,))],
            compiler_params=pltpu.CompilerParams(vmem_limit_bytes=1024 * 1024),
        )(*results)
        return tuple(turned(x) for x in stored)

    spec3, spec2 = P("lat", None, "lon"), P("lat", "lon")
    return jax.shard_map(
        on_device,
        mesh=mesh,
        in_specs=(spec3, spec3, spec3, spec3, spec3, spec3, spec2, spec3, spec2, spec3),
        out_specs=(spec3, spec3),
        check_vma=False,
    )
```

```python
import functools

import jax
import jax.numpy as jnp
from jax import lax
from jax.experimental import pallas as pl
from jax.experimental.pallas import tpu as pltpu
from jax.sharding import PartitionSpec as P

NSUB = 3
C = 640
E = 960
EP = 1024
H = 128
L = 30
MID = L // 2
LP = 32
N = 8 * H
DIRECTIONS = ((-1, -1), (-1, 0), (-1, 1), (0, -1), (0, 1), (1, -1), (1, 0), (1, 1))
F32, BF16 = jnp.float32, jnp.bfloat16
MESH = pl.DeviceIdType.MESH


def split(x):
    high = x.astype(BF16)
    return high, (x - high.astype(F32)).astype(BF16)


def dot(a, b):
    return jnp.dot(a, b, preferred_element_type=F32)


def halves(x):
    return x[:LP] + x[LP:]


def kernel(
    n_lat, n_lon,
    p_hbm, v_hbm, ec_hbm, ce_hbm, sc_hbm, se_hbm, inv_hbm, w_hbm, ss_hbm, cp_hbm,
    p_out, v_out,
    p_in, v_in, ec_in, ce_in, sc_in, se_in, inv_in, w_in, ss_in, cp_in,
    pres, vel, pieces_out, pieces_in,
    pres_hl, vel_hl, pick_c, pick_e, diff, diff_l, weight,
    rows_l, grad_l, vel_l, right, solve_in, solve_mid, coef_a, coef_b, coef_r,
    send_sem, recv_sem,
):
    a, b = lax.axis_index("lat"), lax.axis_index("lon")
    not_first, not_last = a > 0, a < n_lat - 1

    def device_at(p, q):
        return (a + p, lax.rem(b + q + n_lon, n_lon))

    def neighbour(member):
        return device_at(*DIRECTIONS[member])

    core = lax.rem(b, 2)
    cross = 2 * core - 1
    order = (
        (-1, cross, 2 * core), (1, cross, 5 + 2 * core),
        (-1, -cross, 2 - 2 * core), (1, -cross, 7 - 2 * core),
        (-1, 0, 1), (1, 0, 6), (0, cross, 3 + core), (0, -cross, 4 - core),
    )

    sources = (sc_hbm, p_hbm, se_hbm, v_hbm, ec_hbm, inv_hbm, ce_hbm, w_hbm, ss_hbm, cp_hbm)
    targets = (sc_in, p_in, se_in, v_in, ec_in, inv_in, ce_in, w_in, ss_in, cp_in)
    loads = []
    for i, (source, target) in enumerate(zip(sources, targets)):
        if source.ndim == 2:
            view = source
        else:
            view = source.at[0] if source.shape[0] == 1 else source.at[:, 0, :]
        semaphore = send_sem.at[0, i] if i < 2 else send_sem.at[1, i - 2]
        loads.append(pltpu.make_async_copy(view, target, semaphore))
    loads[0].start()
    loads[1].start()

    barrier = pltpu.get_barrier_semaphore()

    def greet(members):
        for member in members:
            pl.semaphore_signal(barrier, inc=1, device_id=neighbour(member), device_id_type=MESH)

    greet((3, 4))
    pl.when(not_first)(lambda: greet((0, 1, 2)))
    pl.when(not_last)(lambda: greet((5, 6, 7)))

    for load in loads[2:]:
        load.start()

    def copy(exchange, turn):
        p, q, member = order[turn]
        return pltpu.make_async_remote_copy(
            src_ref=pieces_out.at[exchange, turn],
            dst_ref=pieces_in.at[exchange, 7 - member],
            send_sem=send_sem.at[exchange % 2, turn],
            recv_sem=recv_sem.at[exchange % 2, 7 - member],
            device_id=device_at(p, q),
            device_id_type=MESH,
        )

    def each(turns, action):
        for turn in turns:
            row = order[turn][0]
            if row == 0:
                action(turn)
            else:
                pl.when(not_first if row < 0 else not_last)(functools.partial(action, turn))

    def send(exchange, turns):
        each(turns, lambda turn: copy(exchange, turn).start())

    def receive(exchange, first, count, target, base):
        for i in range(count):
            pltpu.make_async_remote_copy(
                src_ref=pieces_out.at[exchange, i],
                dst_ref=pieces_in.at[exchange, first + i],
                send_sem=send_sem.at[exchange % 2, i],
                recv_sem=recv_sem.at[exchange % 2, first + i],
                device_id=device_at(0, 1),
                device_id_type=MESH,
            ).wait_recv()
        for i in range(count):
            high, low = split(pieces_in[exchange, first + i])
            cols = pl.ds(pl.multiple_of(base + (first + i) * H, H), H)
            target[:L, cols] = high
            target[LP:LP + L, cols] = low

    ahead_first = 1 - lax.min(lax.rem(a, 4), 1)
    farther = 5 - 5 * ahead_first
    farther_there = jnp.where(ahead_first == 1, not_first, not_last)
    groups = (
        (5 * ahead_first, 3, jnp.where(ahead_first == 1, not_last, not_first)),
        (farther + 1 - core, 2, farther_there),
        (farther + 2 * core, 1, farther_there),
    )

    def receive_group(exchange, group, target, base):
        first, count, there = groups[group]
        pl.when(there)(lambda: receive(exchange, first, count, target, base))

    def group_places(group, base):
        first, count, _ = groups[group]
        return pl.ds(pl.multiple_of(base + first * H, H), count * H)

    def in_blocks(count, build):
        def step(block, carry):
            start = pl.multiple_of(block * H, H)
            base = start.astype(F32)

            def local(places):
                within = places - base
                within = jnp.where((within >= 0.0) & (within < float(H)), within, -1.0)
                return jnp.broadcast_to(within, (16, places.shape[1])).astype(BF16)

            build(start, local)
            return carry

        lax.fori_loop(0, count // H, step, 0)

    def row_numbers(j, width):
        return (lax.broadcasted_iota(jnp.int32, (16, width), 0) + 16 * j).astype(F32).astype(BF16)

    def build_pick(lists_ref, target, own):
        lists = lists_ref[...].astype(F32)

        def either(first, second):
            return jnp.where(core == 0, lists[first:first + 1], lists[second:second + 1])

        picks = jnp.concatenate(
            [either(0, 2), either(5, 7), either(2, 0), either(7, 5),
             lists[1:2], lists[6:7], either(3, 4), either(4, 3)], axis=1)

        def build(start, local):
            here = local(picks)
            one, zero = jnp.ones((16, N), BF16), jnp.zeros((16, N), BF16)
            for j in range(H // 16):
                target[pl.ds(start + 16 * j, 16), :] = jnp.where(row_numbers(j, N) == here, one, zero)

        in_blocks(own, build)

    def build_diff(first, second, target):
        def build(start, local):
            minus, plus = local(first), local(second)
            one, zero = jnp.ones((16, N), BF16), jnp.zeros((16, N), BF16)
            for j in range(H // 16):
                rows = row_numbers(j, N)
                hit = jnp.where(rows == plus, one, zero) - jnp.where(rows == minus, one, zero)
                target[pl.ds(start + 16 * j, 16), :] = hit

        in_blocks(C + N, build)

    def build_weight():
        places = ce_in[...].astype(F32)
        places = jnp.where(places >= E, places + (EP - E), places)
        weights = w_in[...] * ss_in[...]
        place = [places[j:j + 1] for j in range(3)]
        factor = [weights[j:j + 1] for j in range(3)]
        for i, j in ((0, 1), (0, 2), (1, 2)):
            same = place[i] == place[j]
            factor[i] = factor[i] + jnp.where(same, factor[j], 0.0)
            place[j] = jnp.where(same, -1.0, place[j])
        parts = [split(jnp.broadcast_to(x, (16, C))) for x in factor]

        def build(start, local):
            here = [local(x) for x in place]
            zero = jnp.zeros((16, C), BF16)
            for j in range(H // 16):
                rows = row_numbers(j, C)
                high, low = zero, zero
                for where, (part_high, part_low) in zip(here, parts):
                    hit = rows == where
                    high, low = jnp.where(hit, part_high, high), jnp.where(hit, part_low, low)
                weight[pl.ds(start + 16 * j, 16), :C] = high
                weight[pl.ds(start + 16 * j, 16), C:] = low

        in_blocks(EP + N, build)

    def to_columns(x, target):
        for block in range(C // H):
            target[pl.ds(block, LP, stride=8), :] = x[:, block * H:(block + 1) * H]

    def build_solver():
        coupling = jnp.concatenate([cp_in[...], jnp.zeros((LP - L, C), F32)], axis=0)
        to_columns(coupling, solve_in)

        def rows(k):
            return slice(8 * k, 8 * k + 8)

        inverse = None
        for k in range(MID):
            above = solve_in[rows(k), :]
            divisor = 1.0 + above
            if k > 0:
                below = solve_in[rows(k - 1), :]
                divisor = divisor + below - below * (below * inverse)
            inverse = 1.0 / divisor
            coef_a[rows(k), :] = inverse
            if k > 0:
                coef_b[rows(k), :] = below * inverse
            coef_r[rows(k), :] = above * inverse
        inverse = None
        for k in range(L - 1, MID - 1, -1):
            above, below = solve_in[rows(k), :], solve_in[rows(k - 1), :]
            divisor = 1.0 + above + below
            if k < L - 1:
                divisor = divisor - above * (above * inverse)
            inverse = 1.0 / divisor
            coef_a[rows(k), :] = inverse
            if k < L - 1:
                coef_b[rows(k), :] = above * inverse
            coef_r[rows(k), :] = below * inverse
        coef_b[rows(0), :] = 1.0 / (1.0 - coef_r[rows(MID - 1), :] * coef_r[rows(MID), :])

    def solve():
        def rows(k):
            return slice(8 * k, 8 * k + 8)

        low = solve_in[rows(0), :] * coef_a[rows(0), :]
        high = solve_in[rows(L - 1), :] * coef_a[rows(L - 1), :]
        solve_mid[rows(0), :] = low
        solve_mid[rows(L - 1), :] = high
        for k in range(1, MID):
            up, down = rows(k), rows(L - 1 - k)
            low = solve_in[up, :] * coef_a[up, :] + coef_b[up, :] * low
            high = solve_in[down, :] * coef_a[down, :] + coef_b[down, :] * high
            if k < MID - 1:
                solve_mid[up, :] = low
                solve_mid[down, :] = high
        meet = coef_b[rows(0), :]
        low, high = (
            (low + coef_r[rows(MID - 1), :] * high) * meet,
            (high + coef_r[rows(MID), :] * low) * meet,
        )
        solve_mid[rows(MID - 1), :] = low
        solve_mid[rows(MID), :] = high
        for k in range(MID - 2, -1, -1):
            up, down = rows(k), rows(L - 1 - k)
            low = solve_mid[up, :] + coef_r[up, :] * low
            high = solve_mid[down, :] + coef_r[down, :] * high
            solve_mid[up, :] = low
            solve_mid[down, :] = high
        for block in range(C // H):
            x = solve_mid[pl.ds(block, LP, stride=8), :]
            pres[:, block * H:(block + 1) * H] = x
            high, low = split(x)
            pres_hl[:LP, block * H:(block + 1) * H] = high
            pres_hl[LP:, block * H:(block + 1) * H] = low

    def put(exchange, chunks, then=lambda chunk: None):
        for chunk, x in enumerate(chunks):
            for half in range(2):
                pieces_out[exchange, 2 * chunk + half] = x[:L, half * H:(half + 1) * H]
            then(chunk)

    def put_and_send(exchange, chunks):
        put(exchange, chunks, lambda chunk: send(exchange, (2 * chunk, 2 * chunk + 1)))

    def pressure_products():
        products = [dot(pres_hl[:, :C], pick_c[:, chunk * 256:chunk * 256 + 256]) for chunk in range(4)]
        return [halves(x) for x in products]

    def own_gradient():
        for chunk in range(4):
            cols = slice(chunk * 256, chunk * 256 + 256)
            grad_l[:, cols] = halves(dot(pres_hl[:, :C], diff_l[:C, cols]))

    loads[0].wait()
    build_pick(sc_in, pick_c, C)
    loads[1].wait()
    start = jnp.concatenate([p_in[...], jnp.zeros((LP - L, C), F32)], axis=0)
    pres[...] = start
    high, low = split(start)
    pres_hl[:LP, :C] = high
    pres_hl[LP:, :C] = low
    pres_hl[:, C:] = jnp.zeros((2 * LP, N), BF16)
    put(0, pressure_products())
    pl.semaphore_wait(barrier, 2 + 3 * lax.min(a, 1) + 3 * lax.min(n_lat - 1 - a, 1))
    send(0, range(8))

    loads[2].wait()
    build_pick(se_in, pick_e, EP)
    for i in range(3, 10):
        loads[i].wait()
    vel[...] = jnp.zeros_like(vel)
    vel[:L, :E] = v_in[...]
    high, low = split(vel[...])
    vel_hl[:LP, :EP] = high
    vel_hl[LP:, :EP] = low
    vel_hl[:, EP:] = jnp.zeros((2 * LP, N), BF16)
    rows_l[...] = jnp.full(rows_l.shape, -1.0, F32)
    rows_l[0:2, :E] = ec_in[...].astype(F32)
    rows_l[2:3, :] = jnp.zeros((1, EP), F32)
    rows_l[2:3, :E] = 0.5 * inv_in[...]
    own_rows = rows_l[...]
    cells_first, cells_second, factor = own_rows[0:1], own_rows[1:2], own_rows[2:3]
    coarse = jnp.floor(own_rows[0:2] * (1.0 / H))
    fine = own_rows[0:2] - H * coarse
    factor_high = factor.astype(BF16).astype(F32)
    factor_mid = (factor - factor_high).astype(BF16).astype(F32)
    factor_low = factor - factor_high - factor_mid
    parts = jnp.concatenate(
        [coarse, fine, factor_high, factor_mid, factor_low, jnp.zeros((9, EP), F32)], axis=0
    ).astype(BF16)
    for chunk in range(4):
        cols = slice(chunk * 256, chunk * 256 + 256)
        vel_l[:, cols] = halves(dot(vel_hl[:, :EP], pick_e[:, cols]))
        found = dot(parts, pick_e[:, cols])
        rows_l[4:6, cols] = found[0:2] * H + found[2:4]
        rows_l[6:7, cols] = found[4:5] + found[5:6] + found[6:7]
    sent_rows = rows_l[...]
    build_diff(sent_rows[4:5], sent_rows[5:6], diff_l)
    own_gradient()
    build_diff(cells_first, cells_second, diff)

    def substep(s, carry):
        first, second = 2 * s, 2 * s + 1
        receive(first, 3, 2, pres_hl, C)
        receive_group(first, 0, pres_hl, C)
        near, places = slice(C + 3 * H, C + 5 * H), group_places(0, C)
        for chunk in range(4):
            cols = slice(chunk * 256, chunk * 256 + 256)
            sums = dot(pres_hl[:, near], diff_l[near, cols]) + dot(pres_hl[:, places], diff_l[places, cols])
            grad_l[:, cols] = grad_l[:, cols] + halves(sums)
        receive_group(first, 1, pres_hl, C)
        places = group_places(1, C)
        for chunk in range(4):
            cols = slice(chunk * 256, chunk * 256 + 256)
            grad_l[:, cols] = grad_l[:, cols] + halves(dot(pres_hl[:, places], diff_l[places, cols]))
        receive_group(first, 2, pres_hl, C)
        places = group_places(2, C)
        products = [dot(pres_hl[:, places], diff_l[places, chunk * 256:chunk * 256 + 256]) for chunk in range(4)]
        moved = []
        for chunk in range(4):
            cols = slice(chunk * 256, chunk * 256 + 256)
            gradient = grad_l[:, cols] + halves(products[chunk])
            moved.append(vel_l[:, cols] - rows_l[6:7, cols] * gradient)
        put_and_send(second, moved)
        for chunk in range(4):
            vel_l[:, chunk * 256:chunk * 256 + 256] = moved[chunk]

        for chunk in range(4):
            cols = slice(chunk * 256, chunk * 256 + 256)
            gradient = halves(dot(pres_hl[...], diff[:, cols]))
            moved = vel[:, cols] - rows_l[2:3, cols] * gradient
            vel[:, cols] = moved
            high, low = split(moved)
            vel_hl[:LP, cols] = high
            vel_hl[LP:, cols] = low

        @pl.when(s == 0)
        def _():
            build_weight()
            build_solver()

        @pl.when(s == NSUB - 1)
        def _():
            v_out[...] = vel[:L, :E]

        def divergence(*ranges):
            wide = sum(dot(vel_hl[:, places], weight[places, :]) for places in ranges)
            return halves(wide[:, :C] + wide[:, C:])

        right[...] = pres[...] - divergence(slice(0, EP))
        each(range(8), lambda turn: copy(first, turn).wait_send())
        each(range(8), lambda turn: copy(second, turn).wait_send())
        receive(second, 3, 2, vel_hl, EP)
        receive_group(second, 0, vel_hl, EP)
        right[...] = right[...] - divergence(slice(EP + 3 * H, EP + 5 * H), group_places(0, EP))
        receive_group(second, 1, vel_hl, EP)
        right[...] = right[...] - divergence(group_places(1, EP))
        receive_group(second, 2, vel_hl, EP)
        to_columns(right[...] - divergence(group_places(2, EP)), solve_in)
        solve()

        @pl.when(s < NSUB - 1)
        def _():
            put_and_send(second + 1, pressure_products())
            own_gradient()

        return carry

    lax.fori_loop(0, NSUB, substep, 0)
    p_out[...] = pres[:L, :]


def store(p, v, p_out, v_out, sem):
    copies = [
        pltpu.make_async_copy(p, p_out.at[:, 0, :], sem.at[0]),
        pltpu.make_async_copy(v, v_out.at[:, 0, :], sem.at[1]),
    ]
    for copy in copies:
        copy.start()
    for copy in copies:
        copy.wait()


def solution(mesh):
    n_lat, n_lon = mesh.shape["lat"], mesh.shape["lon"]
    any_space = pl.BlockSpec(memory_space=pl.ANY)
    vmem = pltpu.VMEM
    i32 = jnp.int32

    def turned(x):
        return jnp.transpose(x, (1, 0, 2))

    def on_device(p, v, ec, ce, sc, se, inv, w, ss, cp):
        results = pl.pallas_call(
            functools.partial(kernel, n_lat, n_lon),
            out_shape=(
                vmem((L, C), F32),
                vmem((L, E), F32),
            ),
            in_specs=[any_space] * 10,
            out_specs=(pl.BlockSpec(memory_space=vmem),) * 2,
            scratch_shapes=[
                vmem((L, C), F32), vmem((L, E), F32),
                vmem((2, E), i32), vmem((3, C), i32), vmem((8, H), i32), vmem((8, H), i32),
                vmem((1, E), F32), vmem((3, C), F32), vmem((1, C), F32), vmem((L, C), F32),
                vmem((LP, C), F32), vmem((LP, EP), F32),
                vmem((2 * NSUB, 8, L, H), F32), vmem((2 * NSUB, 8, L, H), F32),
                vmem((2 * LP, C + N), BF16), vmem((2 * LP, EP + N), BF16),
                vmem((C, N), BF16), vmem((EP, N), BF16),
                vmem((C + N, N), BF16), vmem((C + N, N), BF16), vmem((EP + N, 2 * C), BF16),
                vmem((8, N), F32), vmem((LP, N), F32), vmem((LP, N), F32), vmem((LP, C), F32),
                vmem((8 * LP, H), F32), vmem((8 * LP, H), F32),
                vmem((8 * LP, H), F32), vmem((8 * LP, H), F32), vmem((8 * LP, H), F32),
                pltpu.SemaphoreType.DMA((2, 8)), pltpu.SemaphoreType.DMA((2, 8)),
            ],
            compiler_params=pltpu.CompilerParams(
                collective_id=0, has_side_effects=True, vmem_limit_bytes=60 * 1024 * 1024
            ),
        )(turned(p), turned(v), ec, turned(ce), sc, se, inv, turned(w), ss, turned(cp))
        stored = pl.pallas_call(
            store,
            out_shape=(
                jax.ShapeDtypeStruct((L, 1, C), F32),
                jax.ShapeDtypeStruct((L, 1, E), F32),
            ),
            in_specs=[pl.BlockSpec(memory_space=vmem)] * 2,
            out_specs=(any_space, any_space),
            scratch_shapes=[pltpu.SemaphoreType.DMA((2,))],
            compiler_params=pltpu.CompilerParams(vmem_limit_bytes=1024 * 1024),
        )(*results)
        return tuple(turned(x) for x in stored)

    spec3, spec2 = P("lat", None, "lon"), P("lat", "lon")
    return jax.shard_map(
        on_device,
        mesh=mesh,
        in_specs=(spec3, spec3, spec3, spec3, spec3, spec3, spec2, spec3, spec2, spec3),
        out_specs=(spec3, spec3),
        check_vma=False,
    )
```

```python
import functools

import jax
import jax.numpy as jnp
from jax import lax
from jax.experimental import pallas as pl
from jax.experimental.pallas import tpu as pltpu
from jax.sharding import PartitionSpec as P

NSUB = 3
C = 640
E = 960
EP = 1024
H = 128
L = 30
MID = L // 2
LP = 32
N = 8 * H
DIRECTIONS = ((-1, -1), (-1, 0), (-1, 1), (0, -1), (0, 1), (1, -1), (1, 0), (1, 1))
F32, BF16 = jnp.float32, jnp.bfloat16
MESH = pl.DeviceIdType.MESH


def split(x):
    high = x.astype(BF16)
    return high, (x - high.astype(F32)).astype(BF16)


def dot(a, b):
    return jnp.dot(a, b, preferred_element_type=F32)


def halves(x):
    return x[:LP] + x[LP:]


def kernel(
    n_lat, n_lon,
    p_hbm, v_hbm, ec_hbm, ce_hbm, sc_hbm, se_hbm, inv_hbm, w_hbm, ss_hbm, cp_hbm,
    p_out, v_out,
    p_in, v_in, ec_in, ce_in, sc_in, se_in, inv_in, w_in, ss_in, cp_in,
    pres, vel, pieces_out, pieces_in,
    pres_hl, vel_hl, pick_c, pick_e, diff, diff_l, weight,
    rows_l, grad_l, vel_l, right, solve_in, solve_mid, coef_a, coef_b, coef_r,
    send_sem, recv_sem,
):
    a, b = lax.axis_index("lat"), lax.axis_index("lon")
    not_first, not_last = a > 0, a < n_lat - 1

    def device_at(p, q):
        return (a + p, lax.rem(b + q + n_lon, n_lon))

    def neighbour(member):
        return device_at(*DIRECTIONS[member])

    core = lax.rem(b, 2)
    cross = 2 * core - 1
    order = (
        (-1, cross, 2 * core), (1, cross, 5 + 2 * core),
        (-1, -cross, 2 - 2 * core), (1, -cross, 7 - 2 * core),
        (-1, 0, 1), (1, 0, 6), (0, cross, 3 + core), (0, -cross, 4 - core),
    )

    sources = (sc_hbm, p_hbm, se_hbm, v_hbm, ec_hbm, inv_hbm, ce_hbm, w_hbm, ss_hbm, cp_hbm)
    targets = (sc_in, p_in, se_in, v_in, ec_in, inv_in, ce_in, w_in, ss_in, cp_in)
    loads = []
    for i, (source, target) in enumerate(zip(sources, targets)):
        if source.ndim == 2:
            view = source
        else:
            view = source.at[0] if source.shape[0] == 1 else source.at[:, 0, :]
        semaphore = send_sem.at[i] if i < 2 else recv_sem.at[1, i - 2]
        loads.append(pltpu.make_async_copy(view, target, semaphore))
    loads[0].start()
    loads[1].start()

    barrier = pltpu.get_barrier_semaphore()

    def greet(members):
        for member in members:
            pl.semaphore_signal(barrier, inc=1, device_id=neighbour(member), device_id_type=MESH)

    greet((3, 4))
    pl.when(not_first)(lambda: greet((0, 1, 2)))
    pl.when(not_last)(lambda: greet((5, 6, 7)))

    for load in loads[2:]:
        load.start()

    def copy(exchange, turn):
        p, q, member = order[turn]
        return pltpu.make_async_remote_copy(
            src_ref=pieces_out.at[exchange, turn],
            dst_ref=pieces_in.at[exchange, 7 - member],
            send_sem=send_sem.at[exchange % 2],
            recv_sem=recv_sem.at[exchange % 2, 7 - member],
            device_id=device_at(p, q),
            device_id_type=MESH,
        )

    def each(turns, action):
        for turn in turns:
            row = order[turn][0]
            if row == 0:
                action(turn)
            else:
                pl.when(not_first if row < 0 else not_last)(functools.partial(action, turn))

    def send(exchange, turns):
        each(turns, lambda turn: copy(exchange, turn).start())

    def receive(exchange, first, count, target, base):
        for i in range(count):
            pltpu.make_async_remote_copy(
                src_ref=pieces_out.at[exchange, i],
                dst_ref=pieces_in.at[exchange, first + i],
                send_sem=send_sem.at[exchange % 2],
                recv_sem=recv_sem.at[exchange % 2, first + i],
                device_id=device_at(0, 1),
                device_id_type=MESH,
            ).wait_recv()
        for i in range(count):
            high, low = split(pieces_in[exchange, first + i])
            cols = pl.ds(pl.multiple_of(base + (first + i) * H, H), H)
            target[:L, cols] = high
            target[LP:LP + L, cols] = low

    ahead_first = 1 - lax.min(lax.rem(a, 4), 1)
    farther = 5 - 5 * ahead_first
    farther_there = jnp.where(ahead_first == 1, not_first, not_last)
    groups = (
        (5 * ahead_first, 3, jnp.where(ahead_first == 1, not_last, not_first)),
        (farther + 1 - core, 2, farther_there),
        (farther + 2 * core, 1, farther_there),
    )

    def receive_group(exchange, group, target, base):
        first, count, there = groups[group]
        pl.when(there)(lambda: receive(exchange, first, count, target, base))

    def group_places(group, base):
        first, count, _ = groups[group]
        return pl.ds(pl.multiple_of(base + first * H, H), count * H)

    def wait_sent(exchange):
        def wait_for(count):
            pltpu.make_async_remote_copy(
                src_ref=pieces_out.at[exchange, pl.ds(0, count)],
                dst_ref=pieces_in.at[exchange, pl.ds(0, count)],
                send_sem=send_sem.at[exchange % 2],
                recv_sem=recv_sem.at[exchange % 2, 0],
                device_id=device_at(0, 1),
                device_id_type=MESH,
            ).wait_send()

        inside = not_first & not_last
        pl.when(inside)(lambda: wait_for(8))
        pl.when(jnp.logical_not(inside))(lambda: wait_for(5 if n_lat > 1 else 2))

    def in_blocks(count, build):
        def step(block, carry):
            start = pl.multiple_of(block * H, H)
            base = start.astype(F32)

            def local(places):
                within = places - base
                within = jnp.where((within >= 0.0) & (within < float(H)), within, -1.0)
                return jnp.broadcast_to(within, (16, places.shape[1])).astype(BF16)

            build(start, local)
            return carry

        lax.fori_loop(0, count // H, step, 0)

    def row_numbers(j, width):
        return (lax.broadcasted_iota(jnp.int32, (16, width), 0) + 16 * j).astype(F32).astype(BF16)

    def build_pick(lists_ref, target, own):
        lists = lists_ref[...].astype(F32)

        def either(first, second):
            return jnp.where(core == 0, lists[first:first + 1], lists[second:second + 1])

        picks = jnp.concatenate(
            [either(0, 2), either(5, 7), either(2, 0), either(7, 5),
             lists[1:2], lists[6:7], either(3, 4), either(4, 3)], axis=1)

        def build(start, local):
            here = local(picks)
            one, zero = jnp.ones((16, N), BF16), jnp.zeros((16, N), BF16)
            for j in range(H // 16):
                target[pl.ds(start + 16 * j, 16), :] = jnp.where(row_numbers(j, N) == here, one, zero)

        in_blocks(own, build)

    def build_diff(first, second, target):
        def build(start, local):
            minus, plus = local(first), local(second)
            one, zero = jnp.ones((16, N), BF16), jnp.zeros((16, N), BF16)
            for j in range(H // 16):
                rows = row_numbers(j, N)
                hit = jnp.where(rows == plus, one, zero) - jnp.where(rows == minus, one, zero)
                target[pl.ds(start + 16 * j, 16), :] = hit

        in_blocks(C + N, build)

    def build_weight():
        places = ce_in[...].astype(F32)
        places = jnp.where(places >= E, places + (EP - E), places)
        weights = w_in[...] * ss_in[...]
        place = [places[j:j + 1] for j in range(3)]
        factor = [weights[j:j + 1] for j in range(3)]
        for i, j in ((0, 1), (0, 2), (1, 2)):
            same = place[i] == place[j]
            factor[i] = factor[i] + jnp.where(same, factor[j], 0.0)
            place[j] = jnp.where(same, -1.0, place[j])
        parts = [split(jnp.broadcast_to(x, (16, C))) for x in factor]

        def build(start, local):
            here = [local(x) for x in place]
            zero = jnp.zeros((16, C), BF16)
            for j in range(H // 16):
                rows = row_numbers(j, C)
                high, low = zero, zero
                for where, (part_high, part_low) in zip(here, parts):
                    hit = rows == where
                    high, low = jnp.where(hit, part_high, high), jnp.where(hit, part_low, low)
                weight[pl.ds(start + 16 * j, 16), :C] = high
                weight[pl.ds(start + 16 * j, 16), C:] = low

        in_blocks(EP + N, build)

    def to_columns(x, target):
        for block in range(C // H):
            target[pl.ds(block, LP, stride=8), :] = x[:, block * H:(block + 1) * H]

    def build_solver():
        coupling = jnp.concatenate([cp_in[...], jnp.zeros((LP - L, C), F32)], axis=0)
        to_columns(coupling, solve_in)

        def rows(k):
            return slice(8 * k, 8 * k + 8)

        inverse = None
        for k in range(MID):
            above = solve_in[rows(k), :]
            divisor = 1.0 + above
            if k > 0:
                below = solve_in[rows(k - 1), :]
                divisor = divisor + below - below * (below * inverse)
            inverse = 1.0 / divisor
            coef_a[rows(k), :] = inverse
            if k > 0:
                coef_b[rows(k), :] = below * inverse
            coef_r[rows(k), :] = above * inverse
        inverse = None
        for k in range(L - 1, MID - 1, -1):
            above, below = solve_in[rows(k), :], solve_in[rows(k - 1), :]
            divisor = 1.0 + above + below
            if k < L - 1:
                divisor = divisor - above * (above * inverse)
            inverse = 1.0 / divisor
            coef_a[rows(k), :] = inverse
            if k < L - 1:
                coef_b[rows(k), :] = above * inverse
            coef_r[rows(k), :] = below * inverse
        coef_b[rows(0), :] = 1.0 / (1.0 - coef_r[rows(MID - 1), :] * coef_r[rows(MID), :])

    def solve():
        def rows(k):
            return slice(8 * k, 8 * k + 8)

        low = solve_in[rows(0), :] * coef_a[rows(0), :]
        high = solve_in[rows(L - 1), :] * coef_a[rows(L - 1), :]
        solve_mid[rows(0), :] = low
        solve_mid[rows(L - 1), :] = high
        for k in range(1, MID):
            up, down = rows(k), rows(L - 1 - k)
            low = solve_in[up, :] * coef_a[up, :] + coef_b[up, :] * low
            high = solve_in[down, :] * coef_a[down, :] + coef_b[down, :] * high
            if k < MID - 1:
                solve_mid[up, :] = low
                solve_mid[down, :] = high
        meet = coef_b[rows(0), :]
        low, high = (
            (low + coef_r[rows(MID - 1), :] * high) * meet,
            (high + coef_r[rows(MID), :] * low) * meet,
        )
        solve_mid[rows(MID - 1), :] = low
        solve_mid[rows(MID), :] = high
        for k in range(MID - 2, -1, -1):
            up, down = rows(k), rows(L - 1 - k)
            low = solve_mid[up, :] + coef_r[up, :] * low
            high = solve_mid[down, :] + coef_r[down, :] * high
            solve_mid[up, :] = low
            solve_mid[down, :] = high
        for block in range(C // H):
            x = solve_mid[pl.ds(block, LP, stride=8), :]
            pres[:, block * H:(block + 1) * H] = x
            high, low = split(x)
            pres_hl[:LP, block * H:(block + 1) * H] = high
            pres_hl[LP:, block * H:(block + 1) * H] = low

    def put(exchange, chunk, x):
        for half in range(2):
            pieces_out[exchange, 2 * chunk + half] = x[:L, half * H:(half + 1) * H]

    def pressure_product(chunk):
        return dot(pres_hl[:, :C], pick_c[:, chunk * 256:chunk * 256 + 256])

    def send_pressure(exchange):
        ready = [pressure_product(0), pressure_product(1)]
        for chunk in range(4):
            put(exchange, chunk, halves(ready[chunk]))
            send(exchange, (2 * chunk, 2 * chunk + 1))
            if chunk == 0:
                ready += [pressure_product(2), pressure_product(3)]

    def own_gradient():
        for chunk in range(4):
            cols = slice(chunk * 256, chunk * 256 + 256)
            grad_l[:, cols] = halves(dot(pres_hl[:, :C], diff_l[:C, cols]))

    loads[0].wait()
    build_pick(sc_in, pick_c, C)
    loads[1].wait()
    start = jnp.concatenate([p_in[...], jnp.zeros((LP - L, C), F32)], axis=0)
    pres[...] = start
    high, low = split(start)
    pres_hl[:LP, :C] = high
    pres_hl[LP:, :C] = low
    pres_hl[:, C:] = jnp.zeros((2 * LP, N), BF16)
    for load in loads[2:]:
        load.wait()
    for chunk in range(4):
        put(0, chunk, halves(pressure_product(chunk)))
    pl.semaphore_wait(barrier, 2 + 3 * lax.min(a, 1) + 3 * lax.min(n_lat - 1 - a, 1))
    send(0, range(8))

    build_pick(se_in, pick_e, EP)
    vel[...] = jnp.zeros_like(vel)
    vel[:L, :E] = v_in[...]
    high, low = split(vel[...])
    vel_hl[:LP, :EP] = high
    vel_hl[LP:, :EP] = low
    vel_hl[:, EP:] = jnp.zeros((2 * LP, N), BF16)
    rows_l[...] = jnp.full(rows_l.shape, -1.0, F32)
    rows_l[0:2, :E] = ec_in[...].astype(F32)
    rows_l[2:3, :] = jnp.zeros((1, EP), F32)
    rows_l[2:3, :E] = 0.5 * inv_in[...]
    own_rows = rows_l[...]
    cells_first, cells_second, factor = own_rows[0:1], own_rows[1:2], own_rows[2:3]
    coarse = jnp.floor(own_rows[0:2] * (1.0 / H))
    fine = own_rows[0:2] - H * coarse
    factor_high = factor.astype(BF16).astype(F32)
    factor_mid = (factor - factor_high).astype(BF16).astype(F32)
    factor_low = factor - factor_high - factor_mid
    parts = jnp.concatenate(
        [coarse, fine, factor_high, factor_mid, factor_low, jnp.zeros((9, EP), F32)], axis=0
    ).astype(BF16)
    for chunk in range(4):
        cols = slice(chunk * 256, chunk * 256 + 256)
        vel_l[:, cols] = halves(dot(vel_hl[:, :EP], pick_e[:, cols]))
        found = dot(parts, pick_e[:, cols])
        rows_l[4:6, cols] = found[0:2] * H + found[2:4]
        rows_l[6:7, cols] = found[4:5] + found[5:6] + found[6:7]
    sent_rows = rows_l[...]
    build_diff(sent_rows[4:5], sent_rows[5:6], diff_l)
    own_gradient()
    build_diff(cells_first, cells_second, diff)

    def substep(s, carry):
        first, second = 2 * s, 2 * s + 1
        receive(first, 3, 2, pres_hl, C)
        receive_group(first, 0, pres_hl, C)
        near, places = slice(C + 3 * H, C + 5 * H), group_places(0, C)
        for chunk in range(4):
            cols = slice(chunk * 256, chunk * 256 + 256)
            sums = dot(pres_hl[:, near], diff_l[near, cols]) + dot(pres_hl[:, places], diff_l[places, cols])
            grad_l[:, cols] = grad_l[:, cols] + halves(sums)
        receive_group(first, 1, pres_hl, C)
        places = group_places(1, C)
        for chunk in range(4):
            cols = slice(chunk * 256, chunk * 256 + 256)
            grad_l[:, cols] = grad_l[:, cols] + halves(dot(pres_hl[:, places], diff_l[places, cols]))
        receive_group(first, 2, pres_hl, C)
        places = group_places(2, C)
        products = [dot(pres_hl[:, places], diff_l[places, chunk * 256:chunk * 256 + 256]) for chunk in range(4)]
        moved = []
        for chunk in range(4):
            cols = slice(chunk * 256, chunk * 256 + 256)
            gradient = grad_l[:, cols] + halves(products[chunk])
            moved.append(vel_l[:, cols] - rows_l[6:7, cols] * gradient)
        for chunk in range(4):
            put(second, chunk, moved[chunk])
            send(second, (2 * chunk, 2 * chunk + 1))
        for chunk in range(4):
            vel_l[:, chunk * 256:chunk * 256 + 256] = moved[chunk]

        for chunk in range(4):
            cols = slice(chunk * 256, chunk * 256 + 256)
            gradient = halves(dot(pres_hl[...], diff[:, cols]))
            moved = vel[:, cols] - rows_l[2:3, cols] * gradient
            vel[:, cols] = moved
            high, low = split(moved)
            vel_hl[:LP, cols] = high
            vel_hl[LP:, cols] = low

        @pl.when(s == 0)
        def _():
            build_weight()
            build_solver()

        @pl.when(s == NSUB - 1)
        def _():
            v_out[...] = vel[:L, :E]

        def divergence(*ranges):
            wide = sum(dot(vel_hl[:, places], weight[places, :]) for places in ranges)
            return halves(wide[:, :C] + wide[:, C:])

        right[...] = pres[...] - divergence(slice(0, EP))
        wait_sent(first)
        wait_sent(second)
        receive(second, 3, 2, vel_hl, EP)
        receive_group(second, 0, vel_hl, EP)
        right[...] = right[...] - divergence(slice(EP + 3 * H, EP + 5 * H), group_places(0, EP))
        receive_group(second, 1, vel_hl, EP)
        right[...] = right[...] - divergence(group_places(1, EP))
        receive_group(second, 2, vel_hl, EP)
        to_columns(right[...] - divergence(group_places(2, EP)), solve_in)
        solve()

        @pl.when(s < NSUB - 1)
        def _():
            send_pressure(second + 1)
            own_gradient()

        return carry

    lax.fori_loop(0, NSUB, substep, 0)
    p_out[...] = pres[:L, :]


def store(p, v, p_out, v_out, sem):
    copies = [
        pltpu.make_async_copy(p, p_out.at[:, 0, :], sem.at[0]),
        pltpu.make_async_copy(v, v_out.at[:, 0, :], sem.at[1]),
    ]
    for copy in copies:
        copy.start()
    for copy in copies:
        copy.wait()


def solution(mesh):
    n_lat, n_lon = mesh.shape["lat"], mesh.shape["lon"]
    any_space = pl.BlockSpec(memory_space=pl.ANY)
    vmem = pltpu.VMEM
    i32 = jnp.int32

    def turned(x):
        return jnp.transpose(x, (1, 0, 2))

    def on_device(p, v, ec, ce, sc, se, inv, w, ss, cp):
        results = pl.pallas_call(
            functools.partial(kernel, n_lat, n_lon),
            out_shape=(
                vmem((L, C), F32),
                vmem((L, E), F32),
            ),
            in_specs=[any_space] * 10,
            out_specs=(pl.BlockSpec(memory_space=vmem),) * 2,
            scratch_shapes=[
                vmem((L, C), F32), vmem((L, E), F32),
                vmem((2, E), i32), vmem((3, C), i32), vmem((8, H), i32), vmem((8, H), i32),
                vmem((1, E), F32), vmem((3, C), F32), vmem((1, C), F32), vmem((L, C), F32),
                vmem((LP, C), F32), vmem((LP, EP), F32),
                vmem((2 * NSUB, 8, L, H), F32), vmem((2 * NSUB, 8, L, H), F32),
                vmem((2 * LP, C + N), BF16), vmem((2 * LP, EP + N), BF16),
                vmem((C, N), BF16), vmem((EP, N), BF16),
                vmem((C + N, N), BF16), vmem((C + N, N), BF16), vmem((EP + N, 2 * C), BF16),
                vmem((8, N), F32), vmem((LP, N), F32), vmem((LP, N), F32), vmem((LP, C), F32),
                vmem((8 * LP, H), F32), vmem((8 * LP, H), F32),
                vmem((8 * LP, H), F32), vmem((8 * LP, H), F32), vmem((8 * LP, H), F32),
                pltpu.SemaphoreType.DMA((2,)), pltpu.SemaphoreType.DMA((2, 8)),
            ],
            compiler_params=pltpu.CompilerParams(
                collective_id=0, has_side_effects=True, vmem_limit_bytes=60 * 1024 * 1024
            ),
        )(turned(p), turned(v), ec, turned(ce), sc, se, inv, turned(w), ss, turned(cp))
        stored = pl.pallas_call(
            store,
            out_shape=(
                jax.ShapeDtypeStruct((L, 1, C), F32),
                jax.ShapeDtypeStruct((L, 1, E), F32),
            ),
            in_specs=[pl.BlockSpec(memory_space=vmem)] * 2,
            out_specs=(any_space, any_space),
            scratch_shapes=[pltpu.SemaphoreType.DMA((2,))],
            compiler_params=pltpu.CompilerParams(vmem_limit_bytes=1024 * 1024),
        )(*results)
        return tuple(turned(x) for x in stored)

    spec3, spec2 = P("lat", None, "lon"), P("lat", "lon")
    return jax.shard_map(
        on_device,
        mesh=mesh,
        in_specs=(spec3, spec3, spec3, spec3, spec3, spec3, spec2, spec3, spec2, spec3),
        out_specs=(spec3, spec3),
        check_vma=False,
    )
```
